32 devices in a mesh: dp: 8 (over z, core), tensor: 4 (over y, x).
Axes of the slice: x: 2, y: 2, z: 4, core: 2. Of those that a mesh axis runs over, the one named last changes fastest.
Arguments:
- tokens: bfloat16 [8192, 2048], P('dp'), may hold values from -6 to 6
- lengths: int32 [8], P('dp'), may hold values from 256 to 1024, as said below
- norm1_gain: bfloat16 [2048], replicated, may hold values from 0.5 to 1.5
- norm1_shift: bfloat16 [2048], replicated, may hold values from -4 to 4
- query_weight: bfloat16 [2048, 2048], P(None, 'tensor'), may hold values from -0.1875 to 0.1875
- query_bias: bfloat16 [2048], P('tensor'), may hold values from -6 to 6
- keyval_weight: bfloat16 [2048, 256], replicated, may hold values from -0.1875 to 0.1875
- value_bias: bfloat16 [128], replicated, may hold values from -6 to 6
- proj_weight: bfloat16 [2048, 2048], P('tensor'), may hold values from -0.5 to 0.5
- proj_bias: bfloat16 [2048], replicated, may hold values from -4 to 4
- norm2_gain: bfloat16 [2048], replicated, may hold values from 0.5 to 1.5
- norm2_shift: bfloat16 [2048], replicated, may hold values from -4 to 4
- up_weight: bfloat16 [2048, 8192], P(None, 'tensor'), may hold values from -0.125 to 0.125
- up_bias: bfloat16 [8192], P('tensor'), may hold values from -6 to 6
- down_weight: bfloat16 [8192, 2048], P('tensor'), may hold values from -0.0625 to 0.0625
- down_bias: bfloat16 [2048], replicated, may hold values from -4 to 4
- cotangent: bfloat16 [8192, 2048], P('dp'), may hold values from -6 to 6
Outputs:
- result: bfloat16 [8192, 2048], P('dp')
- grad_tokens: bfloat16 [8192, 2048], P('dp')
- grad_gain1: float32 [2048], replicated
- grad_shift1: float32 [2048], replicated
- grad_query: float32 [2048, 2048], P(None, 'tensor')
- grad_qbias: float32 [2048], P('tensor')
- grad_keyval: float32 [2048, 256], replicated
- grad_vbias: float32 [128], replicated
- grad_proj: float32 [2048, 2048], P('tensor')
- grad_pbias: float32 [2048], replicated
- grad_gain2: float32 [2048], replicated
- grad_shift2: float32 [2048], replicated
- grad_up: float32 [2048, 8192], P(None, 'tensor')
- grad_upbias: float32 [8192], P('tensor')
- grad_down: float32 [8192, 2048], P('tensor')
- grad_dnbias: float32 [2048], replicated
The draws below stay inside these ranges and needn't reach their ends.
Inputs may be any that keep to these rules, and one draw needn't show every extreme that they name: `lengths`: valid tokens at the start of each slot; some slot is full (1024) and some holds 256.
All inputs are finite; a program needn't handle non-finite values.
Results may differ from the reference program's by a relative error of at most 0.023.
Values may be sent and summed in bfloat16 or wider, within the bound.
A program may use at most 256 MiB of HBM per device.

```python
import jax
import jax.numpy as jnp
from jax import lax

D = 2048
HEADS = 16
HEAD_DIM = 128
FF = 8192
SLOT = 1024
SLOTS = 8
TOKENS = 8192
N_TENSOR = 4


def draw_lengths(key, part):
    key_one = jax.random.fold_in(key, 11)
    key_two = jax.random.fold_in(key, 23)
    spans = jax.random.randint(key_one, (SLOTS,), SLOT // 4, SLOT + 1)
    order = jax.random.permutation(key_two, SLOTS)
    spans = spans.at[order[0]].set(SLOT)
    spans = spans.at[order[1]].set(SLOT // 4)
    return spans.astype(jnp.int32)


def steps_of(key, dims, pieces, smallest, high):
    def one(axis_at, shards_of):
        heights = jax.random.uniform(jax.random.fold_in(jax.random.fold_in(key, 6), axis_at), (shards_of,), jnp.float32, smallest / len(pieces), high / len(pieces))
        return jnp.repeat(jnp.exp(heights), dims[axis_at] // shards_of).reshape((-1,) + (1,) * (len(dims) - axis_at - 1))

    loudness = one(*pieces[0])
    for cut in pieces[1:]:
        loudness = loudness * one(*cut)
    return loudness


def normal_values(key, shape, scale, bound, split=(), kind=jnp.bfloat16):
    loudness = steps_of(key, shape, split, -0.22, 0.18) if split else 1.0
    result = jax.random.normal(key, shape, jnp.float32) * scale * loudness
    return jnp.minimum(jnp.maximum(result, -bound), bound).astype(kind)


def setup_inputs(seed: int = 0) -> dict:
    seeds = jax.random.split(jax.random.key(seed), 18)
    return {
        "tokens": normal_values(seeds[0], (TOKENS, D), 1.0, 6.0, ((0, 8),)),
        "lengths": draw_lengths(jax.random.fold_in(seeds[17], 71), 0),
        "norm1_gain": jnp.clip(1.0 + 0.1 * jax.random.normal(seeds[2], (D,), jnp.float32), 0.5, 1.5).astype(jnp.bfloat16),
        "norm1_shift": normal_values(seeds[3], (D,), 0.3, 4.0),
        "query_weight": normal_values(seeds[4], (D, HEADS * HEAD_DIM), (D // 2) ** -0.5, 0.1875, ((1, 4),)),
        "query_bias": normal_values(seeds[5], (HEADS * HEAD_DIM,), 0.5, 6.0, ((0, 4),)),
        "keyval_weight": normal_values(seeds[6], (D, 2 * HEAD_DIM), (D // 2) ** -0.5, 0.1875),
        "value_bias": normal_values(seeds[7], (HEAD_DIM,), 0.5, 6.0),
        "proj_weight": normal_values(seeds[8], (HEADS * HEAD_DIM, D), HEAD_DIM ** -0.5, 0.5, ((0, 4),)),
        "proj_bias": normal_values(seeds[9], (D,), 0.3, 4.0),
        "norm2_gain": jnp.clip(1.0 + 0.1 * jax.random.normal(seeds[10], (D,), jnp.float32), 0.5, 1.5).astype(jnp.bfloat16),
        "norm2_shift": normal_values(seeds[11], (D,), 0.3, 4.0),
        "up_weight": normal_values(seeds[12], (D, FF), D ** -0.5, 0.125, ((1, 4),)),
        "up_bias": normal_values(seeds[13], (FF,), 0.5, 6.0, ((0, 4),)),
        "down_weight": normal_values(seeds[14], (FF, D), FF ** -0.5, 0.0625, ((0, 4),)),
        "down_bias": normal_values(seeds[15], (D,), 0.3, 4.0),
        "cotangent": normal_values(seeds[16], (TOKENS, D), 1.0, 6.0, ((0, 8),)),
    }


@jax.custom_vjp
def low(v):
    return lax.optimization_barrier(v.astype(jnp.bfloat16)).astype(jnp.float32)

@jax.custom_vjp
def low_back(v):
    return v

def low_keep(v):
    return (low(v), None)

def low_pass(kept, grad):
    return (grad,)

def back_keep(v):
    return (v, None)

def back_low(kept, grad):
    return (low(grad),)
low.defvjp(low_keep, low_pass)
low_back.defvjp(back_keep, back_low)
HIGH = lax.Precision.HIGHEST

def matmul(left, right):
    return jnp.dot(left, right, precision=HIGH, preferred_element_type=jnp.float32)

def layer_norm(values, gain, shift):
    center = values - lax.optimization_barrier(jnp.mean(values, axis=-1, keepdims=True))
    scaled = center * lax.rsqrt(lax.optimization_barrier(jnp.mean(center * center, axis=-1, keepdims=True)) + 1e-05)
    return scaled * gain + shift

def gelu_tanh(values):
    return 0.5 * values * (1.0 + jnp.tanh(0.7978845608028654 * (values + 0.044715 * values * values * values)))

def attend(queries, key_rows, value_rows, length):
    block_rows = min(512, SLOT)
    counter = SLOT // block_rows
    heads_here = queries.shape[1]
    query_blocks = queries.reshape(counter, block_rows, heads_here, HEAD_DIM)
    offsets = jnp.arange(counter, dtype=jnp.int32) * block_rows
    keys_pos = jnp.arange(SLOT, dtype=jnp.int32)

    def one_block(paired):
        query_block, offset = paired
        scores = jnp.einsum('qhd,kd->hqk', query_block, key_rows, precision=HIGH) * HEAD_DIM ** (-0.5)
        scores = low_back(scores)
        rows_pos = offset + jnp.arange(block_rows, dtype=jnp.int32)
        allowed = (keys_pos[None, :] <= rows_pos[:, None]) & (keys_pos[None, :] < length)
        scores = jnp.where(allowed[None], scores, -1e+30)
        highest = lax.optimization_barrier(jnp.max(scores, axis=-1, keepdims=True))
        exponent = jnp.exp(scores - highest)
        probs = low(exponent / lax.optimization_barrier(jnp.sum(exponent, axis=-1, keepdims=True)))
        return jnp.einsum('hqk,kd->qhd', probs, value_rows, precision=HIGH)
    blocks_out = lax.map(jax.checkpoint(one_block), (query_blocks, offsets))
    return blocks_out.reshape(SLOT, heads_here * HEAD_DIM)

def forward(slot_tokens, params, length):
    gain1, shift1, wquery, bquery, wkeyval, bvalue, wproj, bproj, gain2, shift2, wup, bup, wdown, bdown = params
    heads_dev = HEADS // N_TENSOR
    width = heads_dev * HEAD_DIM
    units = FF // N_TENSOR
    normed = low(layer_norm(slot_tokens, gain1, shift1))
    attn_total = jnp.zeros((SLOT, D), jnp.float32)
    for member in range(N_TENSOR):
        local = low_back(normed)
        cols = slice(member * width, (member + 1) * width)
        queries = low_back(low(matmul(local, wquery[:, cols]) + bquery[cols]))
        keyval = matmul(local, wkeyval)
        key_rows = low_back(low(keyval[:, :HEAD_DIM]))
        value_rows = low_back(low(keyval[:, HEAD_DIM:] + bvalue))
        heads_out = low_back(low(attend(queries.reshape(SLOT, heads_dev, HEAD_DIM), key_rows, value_rows, length)))
        attn_total = attn_total + low(matmul(heads_out, wproj[cols, :]))
    middle = slot_tokens + low_back(attn_total) + bproj
    normed2 = low(layer_norm(middle, gain2, shift2))
    mlp_total = jnp.zeros((SLOT, D), jnp.float32)
    for member in range(N_TENSOR):
        local = low_back(normed2)
        cols = slice(member * units, (member + 1) * units)
        pre = low_back(matmul(local, wup[:, cols]) + bup[cols])
        activated = low_back(low(gelu_tanh(pre)))
        mlp_total = mlp_total + low(matmul(activated, wdown[cols, :]))
    return middle + low_back(mlp_total) + bdown

def reference(tokens, lengths, norm1_gain, norm1_shift, query_weight, query_bias, keyval_weight, value_bias, proj_weight, proj_bias, norm2_gain, norm2_shift, up_weight, up_bias, down_weight, down_bias, cotangent):
    raw = (norm1_gain, norm1_shift, query_weight, query_bias, keyval_weight, value_bias, proj_weight, proj_bias, norm2_gain, norm2_shift, up_weight, up_bias, down_weight, down_bias)
    params = jax.tree.map(lambda weight: weight.astype(jnp.float32), raw)
    slot_inputs = tokens.astype(jnp.float32).reshape(SLOTS, SLOT, D)
    slot_cots = cotangent.astype(jnp.float32).reshape(SLOTS, SLOT, D)

    def per_slot(totals, items):
        slot_tokens, slot_cot, length = items
        valid = (jnp.arange(SLOT, dtype=jnp.int32) < length).astype(jnp.float32)[:, None]
        outcome, pullback = jax.vjp(lambda inputs, weights: forward(inputs, weights, length), slot_tokens, params)
        grad_inputs, grad_params = pullback(slot_cot * valid)
        totals = jax.tree.map(lambda total, extra: total + extra, totals, grad_params)
        return (totals, (outcome.astype(jnp.bfloat16), grad_inputs.astype(jnp.bfloat16)))
    zeros = jax.tree.map(jnp.zeros_like, params)
    totals, (outcomes, grad_inputs) = lax.scan(per_slot, zeros, (slot_inputs, slot_cots, lengths))
    return (outcomes.reshape(TOKENS, D), grad_inputs.reshape(TOKENS, D), totals[0], totals[1], totals[2], totals[3], totals[4], totals[5], totals[6], totals[7], totals[8], totals[9], totals[10], totals[11], totals[12], totals[13])
```

```python
import functools

import jax
import jax.numpy as jnp
from jax import lax
from jax.experimental import pallas as pl
from jax.experimental.pallas import tpu as pltpu
from jax.sharding import PartitionSpec as P

STRIP = 16
SUBS = 2
EPS = 1e-05


def suffixes(count):
    if count == 0:
        return [()]
    rest = [()]
    for _ in range(count - 1):
        rest = [(bit,) + more for bit in (1, 0) for more in rest]
    return [(bit,) + more for bit in (1, 0) for more in rest]


def as_number(path):
    total = 0
    for bit in path:
        total = 2 * total + bit
    return total


class Tree:
    def __init__(self, axis, size, number, rows):
        self.axis, self.size = axis, size
        self.depth = size.bit_length() - 1
        self.number = number
        self.half = rows // 2
        self.unit = self.half // size
        order = list(range(self.depth))
        self.order = order if number == 0 else order[::-1]
        me = lax.axis_index(axis)
        self.mine = [(me // (1 << bit)) % 2 for bit in self.order]
        self.partners = [me + (1 - 2 * own) * (1 << bit) for own, bit in zip(self.mine, self.order)]

    def offset(self, path, skip=0):
        start = 0
        for level in range(skip, self.depth):
            side = (self.mine[level] + path[level]) % 2
            start = start + side * (self.half >> (level + 1))
        return start

    def rows(self, path, sub, sub_rows):
        start = self.number * self.half + self.offset(path) + sub * sub_rows
        return pl.ds(pl.multiple_of(start, sub_rows), sub_rows)

    def own_rows(self, path, sub, sub_rows):
        start = self.offset(path, 1) + sub * sub_rows
        return pl.multiple_of(start, sub_rows)

    def slot(self, level, path):
        base = sum(1 << (self.depth - 1 - lower) for lower in range(level))
        return base + as_number(path)


def stream(axis, size, shape, part, out, own, slots, outbuf, local_sem, send_sem, recv_sem, finish, loads=()):
    rows, width = shape
    trees = [Tree(axis, size, number, rows) for number in (0, 1)]
    unit = trees[0].unit
    depth = trees[0].depth
    sub_rows = unit // SUBS
    sends = []

    def remote(tree, src, dst, kind, index, sub, level):
        place = ((tree.number * 2 + kind) * (size - 1) + index) * SUBS + sub
        copy = pltpu.make_async_remote_copy(
            src_ref=src,
            dst_ref=dst,
            send_sem=send_sem.at[place],
            recv_sem=recv_sem.at[place],
            device_id={axis: tree.partners[level]},
            device_id_type=pl.DeviceIdType.MESH,
        )
        return copy

    def reduce_copy(tree, level, path, sub):
        slot = tree.slot(level, path)
        if level == 0:
            src = part.at[tree.rows((1,) + path, sub, sub_rows), :]
        else:
            src = slots.at[tree.number, tree.slot(level - 1, (1,) + path), pl.ds(sub * sub_rows, sub_rows), :]
        dst = slots.at[tree.number, slot, pl.ds(sub * sub_rows, sub_rows), :]
        return remote(tree, src, dst, 0, slot, sub, level)

    def gather_copy(tree, level, path, sub):
        there = path[:level] + (1,) + path[level + 1 :]
        where = tree.rows(path, sub, sub_rows)
        if any(path):
            src = out.at[where, :]
        else:
            src = outbuf.at[tree.number, pl.ds(sub * sub_rows, sub_rows), :]
        return remote(tree, src, out.at[where, :], 1, as_number(there) - 1, sub, level)

    copies = []
    for tree in trees:
        start = tree.number * tree.half + tree.mine[0] * (tree.half // 2)
        copies.append(
            pltpu.make_async_copy(
                part.at[pl.ds(pl.multiple_of(start, tree.half // 2), tree.half // 2), :],
                own.at[tree.number],
                local_sem.at[tree.number],
            )
        )
    for copy in copies:
        copy.start()
    for path in suffixes(depth - 1):
        for sub in range(SUBS):
            for tree in trees:
                copy = reduce_copy(tree, 0, path, sub)
                copy.start()
                sends.append(copy)
    for copy in copies:
        copy.wait()
    yield
    zero = (0,) * depth
    stored = []
    for level in range(depth):
        last = level == depth - 1
        if last:
            for load in loads:
                load.wait()
        for path in suffixes(depth - 1 - level):
            for sub in range(SUBS):
                for tree in trees:
                    reduce_copy(tree, level, path, sub).wait_recv()
                    slot = tree.slot(level, path)
                    first = tree.own_rows((0,) + path if level == 0 else zero, sub, sub_rows)

                    def strip(step, tree=tree, slot=slot, first=first, path=path, sub=sub, level=level, last=last):
                        line = sub * sub_rows + step * STRIP
                        here = pl.ds(pl.multiple_of(line, STRIP), STRIP)
                        if level == 0:
                            mine = own[tree.number, pl.ds(pl.multiple_of(first + step * STRIP, STRIP), STRIP), :]
                        else:
                            mine = slots[tree.number, tree.slot(level - 1, (0,) + path), here, :]
                        total = mine.astype(jnp.float32) + slots[tree.number, slot, here, :].astype(jnp.float32)
                        if last:
                            outbuf[tree.number, here, :] = finish(
                                total, tree.number, here, pl.ds(pl.multiple_of(tree.number * unit + line, STRIP), STRIP)
                            )
                        else:
                            slots[tree.number, slot, here, :] = total.astype(slots.dtype)

                    pl.loop(0, sub_rows // STRIP)(strip)
                    if last:
                        keep = pltpu.make_async_copy(
                            outbuf.at[tree.number, pl.ds(sub * sub_rows, sub_rows), :],
                            out.at[tree.rows(zero, sub, sub_rows), :],
                            local_sem.at[2 + tree.number * SUBS + sub],
                        )
                        keep.start()
                        stored.append(keep)
                        for back in reversed(range(depth)):
                            copy = gather_copy(tree, back, zero, sub)
                            copy.start()
                            sends.append(copy)
                    elif path[0] == 1:
                        copy = reduce_copy(tree, level + 1, path[1:], sub)
                        copy.start()
                        sends.append(copy)
            if not last:
                yield
        yield
    for level in reversed(range(depth)):
        for path in suffixes(depth - 1 - level):
            full = (0,) * level + (1,) + path
            sender = (0,) * (level + 1) + path
            for sub in range(SUBS):
                for tree in trees:
                    gather_copy(tree, level, sender, sub).wait_recv()
                    for back in reversed(range(level)):
                        copy = gather_copy(tree, back, full, sub)
                        copy.start()
                        sends.append(copy)
        yield
    for copy in sends:
        copy.wait_send()
    for copy in stored:
        copy.wait()


def greet(axis, size):
    barrier = pltpu.get_barrier_semaphore()
    me = lax.axis_index(axis)
    for step in range(1, size):
        pl.semaphore_signal(
            barrier, inc=1, device_id={axis: (me + step) % size}, device_id_type=pl.DeviceIdType.MESH
        )
    pl.semaphore_wait(barrier, size - 1)


def run_together(streams):
    waiting = list(streams)
    while waiting:
        left = []
        for one in waiting:
            try:
                next(one)
                left.append(one)
            except StopIteration:
                pass
        waiting = left


def stream_scratch(size, rows, width):
    half = rows // 2
    unit = half // size
    count = 2 * 2 * (size - 1) * SUBS
    return [
        pltpu.VMEM((2, half // 2, width), jnp.bfloat16),
        pltpu.VMEM((2, size - 1, unit, width), jnp.bfloat16),
        pltpu.VMEM((2, unit, width), jnp.bfloat16),
        pltpu.SemaphoreType.DMA((2 + 2 * SUBS,)),
        pltpu.SemaphoreType.DMA((count,)),
        pltpu.SemaphoreType.DMA((count,)),
    ]


def load_rows(axis, size, rows, source, target, sems):
    copies = []
    for number in (0, 1):
        tree = Tree(axis, size, number, rows)
        unit = tree.unit
        copies.append(
            pltpu.make_async_copy(
                source.at[tree.rows((0,) * tree.depth, 0, unit), :], target.at[number], sems.at[number]
            )
        )
    for copy in copies:
        copy.start()
    return copies


def moments(values):
    center = values - jnp.mean(values, axis=-1, keepdims=True)
    scale = lax.rsqrt(jnp.mean(center * center, axis=-1, keepdims=True) + EPS)
    return center * scale, scale


def norm_back(grad, gain, scaled, scale):
    inner = grad * gain
    return scale * (
        inner
        - jnp.mean(inner, axis=-1, keepdims=True)
        - scaled * jnp.mean(inner * scaled, axis=-1, keepdims=True)
    )


def fold(values):
    return values[:8] + values[8:]


HBM = pl.BlockSpec(memory_space=pl.ANY)
VMEM = pl.BlockSpec(memory_space=pltpu.VMEM)


def middle_kernel(size, rows, width, part, tokens, pbias, gain, shift, hidden, mid, own, slots, outbuf, local_sem, send_sem, recv_sem, tok, load_sem):
    greet("tensor", size)
    loads = load_rows("tensor", size, rows, tokens, tok, load_sem)

    def finish(total, number, here, line):
        value = tok[number, here, :].astype(jnp.float32) + total + pbias[...]
        mid[line, :] = value
        scaled, _ = moments(value)
        return (scaled * gain[...] + shift[...]).astype(jnp.bfloat16)

    run_together(
        [stream("tensor", size, (rows, width), part, hidden, own, slots, outbuf, local_sem, send_sem, recv_sem, finish, loads)]
    )


def reduce_middle(size, part, tokens, pbias, gain, shift):
    rows, width = part.shape
    unit = rows // 2 // size
    return pl.pallas_call(
        functools.partial(middle_kernel, size, rows, width),
        out_shape=(
            jax.ShapeDtypeStruct((rows, width), jnp.bfloat16),
            jax.ShapeDtypeStruct((2 * unit, width), jnp.float32),
        ),
        in_specs=[HBM, HBM, VMEM, VMEM, VMEM],
        out_specs=(HBM, VMEM),
        scratch_shapes=stream_scratch(size, rows, width)
        + [pltpu.VMEM((2, unit, width), jnp.bfloat16), pltpu.SemaphoreType.DMA((2,))],
        compiler_params=pltpu.CompilerParams(collective_id=1, has_side_effects=True),
        name="reduce_middle",
    )(part, tokens, pbias, gain, shift)


def back_kernel(size, rows, width, part, d_out, mid, gain, low, dmid, sums, own, slots, outbuf, local_sem, send_sem, recv_sem, dout, load_sem):
    greet("tensor", size)
    loads = load_rows("tensor", size, rows, d_out, dout, load_sem)
    sums[...] = jnp.zeros_like(sums)

    def finish(total, number, here, line):
        scaled, scale = moments(mid[line, :])
        direct = dout[number, here, :].astype(jnp.float32)
        value = direct + norm_back(total, gain[...], scaled, scale)
        dmid[line, :] = value
        sums[0] += fold(total * scaled)
        sums[1] += fold(total)
        sums[2] += fold(value)
        sums[3] += fold(direct)
        return value.astype(jnp.bfloat16)

    run_together(
        [stream("tensor", size, (rows, width), part, low, own, slots, outbuf, local_sem, send_sem, recv_sem, finish, loads)]
    )


def reduce_back(size, part, d_out, mid, gain):
    rows, width = part.shape
    unit = rows // 2 // size
    return pl.pallas_call(
        functools.partial(back_kernel, size, rows, width),
        out_shape=(
            jax.ShapeDtypeStruct((rows, width), jnp.bfloat16),
            jax.ShapeDtypeStruct((2 * unit, width), jnp.float32),
            jax.ShapeDtypeStruct((4, 8, width), jnp.float32),
        ),
        in_specs=[HBM, HBM, VMEM, VMEM],
        out_specs=(HBM, VMEM, VMEM),
        scratch_shapes=stream_scratch(size, rows, width)
        + [pltpu.VMEM((2, unit, width), jnp.bfloat16), pltpu.SemaphoreType.DMA((2,))],
        compiler_params=pltpu.CompilerParams(collective_id=2, has_side_effects=True),
        name="reduce_back",
    )(part, d_out, mid, gain)


def last_kernel(size, rows, width, kv_rows, mlp, part, kv, tokens, mid, dmid, dbias, gain, result, grad, kv_out, sums, *scratch):
    greet("tensor", size)
    first, second, third = scratch[:6], scratch[6:12], scratch[12:18]
    tok, load_sem = scratch[18:]
    loads = load_rows("tensor", size, rows, tokens, tok, load_sem)
    sums[...] = jnp.zeros_like(sums)

    def finish_result(total, number, here, line):
        return (mid[line, :] + total + dbias[...]).astype(jnp.bfloat16)

    def finish_grad(total, number, here, line):
        scaled, scale = moments(tok[number, here, :].astype(jnp.float32))
        sums[0] += fold(total * scaled)
        sums[1] += fold(total)
        return (dmid[line, :] + norm_back(total, gain[...], scaled, scale)).astype(jnp.bfloat16)

    def finish_kv(total, number, here, line):
        return total.astype(jnp.bfloat16)

    run_together(
        [
            stream("tensor", size, (rows, width), mlp, result, *first, finish_result),
            stream("tensor", size, (rows, width), part, grad, *second, finish_grad, loads),
            stream("tensor", size, (kv_rows, width), kv, kv_out, *third, finish_kv),
        ]
    )


def reduce_last(size, mlp, part, kv, tokens, mid, dmid, dbias, gain):
    rows, width = part.shape
    unit = rows // 2 // size
    kv_rows = kv.shape[0]
    return pl.pallas_call(
        functools.partial(last_kernel, size, rows, width, kv_rows),
        out_shape=(
            jax.ShapeDtypeStruct((rows, width), jnp.bfloat16),
            jax.ShapeDtypeStruct((rows, width), jnp.bfloat16),
            jax.ShapeDtypeStruct((kv_rows, width), jnp.bfloat16),
            jax.ShapeDtypeStruct((2, 8, width), jnp.float32),
        ),
        in_specs=[HBM, HBM, HBM, HBM, VMEM, VMEM, VMEM, VMEM],
        out_specs=(HBM, HBM, HBM, VMEM),
        scratch_shapes=stream_scratch(size, rows, width) * 2
        + stream_scratch(size, kv_rows, width)
        + [pltpu.VMEM((2, unit, width), jnp.bfloat16), pltpu.SemaphoreType.DMA((2,))],
        compiler_params=pltpu.CompilerParams(collective_id=3, has_side_effects=True),
        name="reduce_last",
    )(mlp, part, kv, tokens, mid, dmid, dbias, gain)


def layer_norm(values, gain, shift):
    center = values - jnp.mean(values, axis=-1, keepdims=True)
    scaled = center * lax.rsqrt(jnp.mean(center * center, axis=-1, keepdims=True) + 1e-05)
    return scaled * gain + shift


def gelu_tanh(values):
    return (
        0.5
        * values
        * (1.0 + jnp.tanh(0.7978845608028654 * (values + 0.044715 * values * values * values)))
    )


def contract_rows(left, right):
    return lax.dot_general(
        left, right, (((0,), (0,)), ((), ())), preferred_element_type=jnp.float32
    )


def contract_cols(left, right):
    return lax.dot_general(
        left, right, (((1,), (1,)), ((), ())), preferred_element_type=jnp.float32
    )


def block_scores(query_block, key_rows, offset, length):
    scale = query_block.shape[2] ** (-0.5)
    scores = (
        jnp.einsum("qhd,kd->hqk", query_block, key_rows, preferred_element_type=jnp.float32) * scale
    )
    rows_pos = offset + jnp.arange(query_block.shape[0], dtype=jnp.int32)
    keys_pos = jnp.arange(key_rows.shape[0], dtype=jnp.int32)
    allowed = (keys_pos[None, :] <= rows_pos[:, None]) & (keys_pos[None, :] < length)
    return jnp.where(allowed[None], scores, -1e30)


def attend_forward(queries, key_rows, value_rows, length, block_rows):
    pieces = []
    log_totals = []
    for offset in range(0, queries.shape[0], block_rows):
        query_block = queries[offset : offset + block_rows]
        scores = block_scores(query_block, key_rows, offset, length)
        highest = jnp.max(scores, axis=-1, keepdims=True)
        exponent = jnp.exp(scores - highest)
        normaliser = jnp.sum(exponent, axis=-1, keepdims=True)
        probability = (exponent / normaliser).astype(jnp.bfloat16)
        log_totals.append(highest + jnp.log(normaliser))
        pieces.append(
            jnp.einsum("hqk,kd->qhd", probability, value_rows, preferred_element_type=jnp.float32)
        )
    return (jnp.concatenate(pieces, axis=0), log_totals)


def attend_backward(queries, key_rows, value_rows, length, block_rows, log_totals, grad_heads):
    scale = queries.shape[2] ** (-0.5)
    query_grads = []
    key_grads = jnp.zeros(key_rows.shape, jnp.float32)
    value_grads = jnp.zeros(value_rows.shape, jnp.float32)
    for counter, offset in enumerate(range(0, queries.shape[0], block_rows)):
        query_block = queries[offset : offset + block_rows]
        grad_block = grad_heads[offset : offset + block_rows]
        scores = block_scores(query_block, key_rows, offset, length)
        probability = jnp.exp(scores - log_totals[counter])
        grad_probs = jnp.einsum(
            "qhd,kd->hqk", grad_block, value_rows, preferred_element_type=jnp.float32
        )
        inner = jnp.sum(probability * grad_probs, axis=-1, keepdims=True)
        grad_scores = (probability * (grad_probs - inner)).astype(jnp.bfloat16)
        query_grads.append(
            (
                jnp.einsum("hqk,kd->qhd", grad_scores, key_rows, preferred_element_type=jnp.float32)
                * scale
            ).astype(jnp.bfloat16)
        )
        key_grads = (
            key_grads
            + jnp.einsum(
                "hqk,qhd->kd", grad_scores, query_block, preferred_element_type=jnp.float32
            )
            * scale
        )
        value_grads = value_grads + jnp.einsum(
            "hqk,qhd->kd",
            probability.astype(jnp.bfloat16),
            grad_block,
            preferred_element_type=jnp.float32,
        )
    return (jnp.concatenate(query_grads, axis=0), key_grads, value_grads)


def local(
    size,
    tokens,
    lengths,
    norm1_gain,
    norm1_shift,
    query_weight,
    query_bias,
    keyval_weight,
    value_bias,
    proj_weight,
    proj_bias,
    norm2_gain,
    norm2_shift,
    up_weight,
    up_bias,
    down_weight,
    down_bias,
    cotangent,
):
    wide = jnp.float32
    slot_len, width = tokens.shape
    head_dim = keyval_weight.shape[1] // 2
    heads_here = query_weight.shape[1] // head_dim
    block_rows = min(512, slot_len)
    length = lengths[0]

    def row(vector):
        return vector.astype(wide).reshape(1, -1)

    hidden1 = layer_norm(tokens.astype(wide), norm1_gain.astype(wide), norm1_shift.astype(wide)).astype(jnp.bfloat16)
    queries = (
        jnp.dot(hidden1, query_weight, preferred_element_type=wide) + query_bias.astype(wide)
    ).astype(jnp.bfloat16)
    keyval = jnp.dot(hidden1, keyval_weight, preferred_element_type=wide)
    key_rows = keyval[:, :head_dim].astype(jnp.bfloat16)
    value_rows = (keyval[:, head_dim:] + value_bias.astype(wide)).astype(jnp.bfloat16)
    slot_queries = queries.reshape(slot_len, heads_here, head_dim)
    attended, log_totals = attend_forward(slot_queries, key_rows, value_rows, length, block_rows)
    heads_out = attended.reshape(slot_len, heads_here * head_dim).astype(jnp.bfloat16)
    attn_terms = jnp.dot(heads_out, proj_weight, preferred_element_type=wide).astype(jnp.bfloat16)
    hidden2, mid = reduce_middle(size, attn_terms, tokens, row(proj_bias), row(norm2_gain), row(norm2_shift))

    pre_act = jnp.dot(hidden2, up_weight, preferred_element_type=wide) + up_bias.astype(wide)
    activated = gelu_tanh(pre_act).astype(jnp.bfloat16)
    valid = (jnp.arange(slot_len, dtype=jnp.int32) < length)[:, None]
    d_out = jnp.where(valid, cotangent, jnp.zeros_like(cotangent))
    grad_down = contract_rows(activated, d_out).astype(jnp.bfloat16)
    grad_down = lax.psum(grad_down, "dp")
    grad_act = contract_cols(d_out, down_weight).astype(jnp.bfloat16)
    gelu_pull = jax.vjp(gelu_tanh, pre_act)[1]
    grad_pre = gelu_pull(grad_act.astype(wide))[0].astype(jnp.bfloat16)
    back2 = contract_cols(grad_pre, up_weight).astype(jnp.bfloat16)
    middle_low, dmid, sums2 = reduce_back(size, back2, d_out, mid, row(norm2_gain))
    grad_up = contract_rows(hidden2, grad_pre).astype(jnp.bfloat16)
    grad_up, grad_down = lax.optimization_barrier((grad_up, grad_down))
    grad_up = lax.psum(grad_up, "dp")
    grad_upbias = jnp.sum(grad_pre.astype(wide), axis=0)
    mlp_terms = jnp.dot(activated, down_weight, preferred_element_type=wide).astype(jnp.bfloat16)

    grad_proj = contract_rows(heads_out, middle_low).astype(jnp.bfloat16)
    grad_heads = contract_cols(middle_low, proj_weight).astype(jnp.bfloat16)
    slot_grads = grad_heads.reshape(slot_len, heads_here, head_dim)
    query_part, key_part, value_part = attend_backward(
        slot_queries, key_rows, value_rows, length, block_rows, log_totals, slot_grads
    )
    grad_queries = query_part.reshape(slot_len, heads_here * head_dim)
    grad_kv_rows = jnp.concatenate([key_part, value_part], axis=1).astype(jnp.bfloat16)
    grad_qbias = jnp.sum(grad_queries.astype(wide), axis=0)
    grad_query = contract_rows(hidden1, grad_queries).astype(jnp.bfloat16)
    grad_keyval = contract_rows(hidden1, grad_kv_rows).astype(jnp.bfloat16)
    grad_vbias = jnp.sum(grad_kv_rows[:, head_dim:].astype(wide), axis=0)
    back1 = (
        contract_cols(grad_queries, query_weight) + contract_cols(grad_kv_rows, keyval_weight)
    ).astype(jnp.bfloat16)
    result, grad_tokens, kv_sum, sums1 = reduce_last(
        size,
        mlp_terms,
        back1,
        grad_keyval.reshape(-1, width),
        tokens,
        mid,
        dmid,
        row(down_bias),
        row(norm1_gain),
    )
    grad_query, grad_up = lax.optimization_barrier((grad_query, grad_up))
    grad_query, grad_proj, kv_sum = lax.psum((grad_query, grad_proj, kv_sum), "dp")
    shared = jnp.concatenate(
        [jnp.sum(sums1, axis=1).reshape(-1), jnp.sum(sums2, axis=1).reshape(-1), grad_vbias]
    )
    shared = lax.psum(shared, ("dp", "tensor"))
    split = lax.psum(jnp.concatenate([grad_qbias, grad_upbias]), "dp")
    grad_qbias, grad_upbias = split[: grad_qbias.shape[0]], split[grad_qbias.shape[0] :]
    grad_gain1, grad_shift1, grad_gain2, grad_shift2, grad_pbias, grad_dnbias = (
        shared[place * width : (place + 1) * width] for place in range(6)
    )
    grad_vbias = shared[6 * width :]
    return (
        result,
        grad_tokens,
        grad_gain1,
        grad_shift1,
        grad_query.astype(wide),
        grad_qbias,
        kv_sum.reshape(keyval_weight.shape).astype(wide),
        grad_vbias,
        grad_proj.astype(wide),
        grad_pbias,
        grad_gain2,
        grad_shift2,
        grad_up.astype(wide),
        grad_upbias,
        grad_down.astype(wide),
        grad_dnbias,
    )


def solution(mesh):
    in_specs = (
        P("dp", None),
        P("dp"),
        P(),
        P(),
        P(None, "tensor"),
        P("tensor"),
        P(),
        P(),
        P("tensor", None),
        P(),
        P(),
        P(),
        P(None, "tensor"),
        P("tensor"),
        P("tensor", None),
        P(),
        P("dp", None),
    )
    out_specs = (
        P("dp", None),
        P("dp", None),
        P(),
        P(),
        P(None, "tensor"),
        P("tensor"),
        P(),
        P(),
        P("tensor", None),
        P(),
        P(),
        P(),
        P(None, "tensor"),
        P("tensor"),
        P("tensor", None),
        P(),
    )
    return jax.shard_map(functools.partial(local, mesh.shape["tensor"]), mesh=mesh, in_specs=in_specs, out_specs=out_specs, check_vma=False)
```

```python
import functools

import jax
import jax.numpy as jnp
from jax import lax
from jax.experimental import pallas as pl
from jax.experimental.pallas import tpu as pltpu
from jax.sharding import PartitionSpec as P

STRIP = 16
EPS = 1e-05


def suffixes(count):
    if count == 0:
        return [()]
    rest = [()]
    for _ in range(count - 1):
        rest = [(bit,) + more for bit in (1, 0) for more in rest]
    return [(bit,) + more for bit in (1, 0) for more in rest]


def pieces(unit):
    return 2 if unit % (2 * STRIP) == 0 else 1


def as_number(path):
    total = 0
    for bit in path:
        total = 2 * total + bit
    return total


class Tree:
    def __init__(self, axis, size, number, rows):
        self.axis, self.size = axis, size
        self.depth = size.bit_length() - 1
        self.number = number
        self.half = rows // 2
        self.unit = self.half // size
        order = list(range(self.depth))
        self.order = order if number == 0 else order[::-1]
        me = lax.axis_index(axis)
        self.mine = [(me // (1 << bit)) % 2 for bit in self.order]
        self.partners = [me + (1 - 2 * own) * (1 << bit) for own, bit in zip(self.mine, self.order)]

    def offset(self, path, skip=0):
        start = 0
        for level in range(skip, self.depth):
            side = (self.mine[level] + path[level]) % 2
            start = start + side * (self.half >> (level + 1))
        return start

    def rows(self, path, sub, sub_rows):
        start = self.number * self.half + self.offset(path) + sub * sub_rows
        return pl.ds(pl.multiple_of(start, sub_rows), sub_rows)

    def own_rows(self, path, sub, sub_rows):
        start = self.offset(path, 1) + sub * sub_rows
        return pl.multiple_of(start, sub_rows)

    def slot(self, level, path):
        base = sum(1 << (self.depth - 1 - lower) for lower in range(level))
        return base + as_number(path)


def stream(axis, size, shape, part, out, own, slots, outbuf, local_sem, send_sem, recv_sem, finish, loads=()):
    rows, width = shape
    trees = [Tree(axis, size, number, rows) for number in (0, 1)]
    unit = trees[0].unit
    depth = trees[0].depth
    subs = pieces(unit)
    sub_rows = unit // subs
    sends = []

    def remote(tree, src, dst, kind, index, sub, level):
        place = ((tree.number * 2 + kind) * (size - 1) + index) * subs + sub
        copy = pltpu.make_async_remote_copy(
            src_ref=src,
            dst_ref=dst,
            send_sem=send_sem.at[place],
            recv_sem=recv_sem.at[place],
            device_id={axis: tree.partners[level]},
            device_id_type=pl.DeviceIdType.MESH,
        )
        return copy

    def reduce_copy(tree, level, path, sub):
        slot = tree.slot(level, path)
        if level == 0:
            src = part.at[tree.rows((1,) + path, sub, sub_rows), :]
        else:
            src = slots.at[tree.number, tree.slot(level - 1, (1,) + path), pl.ds(sub * sub_rows, sub_rows), :]
        dst = slots.at[tree.number, slot, pl.ds(sub * sub_rows, sub_rows), :]
        return remote(tree, src, dst, 0, slot, sub, level)

    def gather_copy(tree, level, path, sub):
        there = path[:level] + (1,) + path[level + 1 :]
        where = tree.rows(path, sub, sub_rows)
        if any(path):
            src = out.at[where, :]
        else:
            src = outbuf.at[tree.number, pl.ds(sub * sub_rows, sub_rows), :]
        return remote(tree, src, out.at[where, :], 1, as_number(there) - 1, sub, level)

    copies = []
    for tree in trees:
        start = tree.number * tree.half + tree.mine[0] * (tree.half // 2)
        copies.append(
            pltpu.make_async_copy(
                part.at[pl.ds(pl.multiple_of(start, tree.half // 2), tree.half // 2), :],
                own.at[tree.number],
                local_sem.at[tree.number],
            )
        )
    for copy in copies:
        copy.start()
    for path in suffixes(depth - 1):
        for sub in range(subs):
            for tree in trees:
                copy = reduce_copy(tree, 0, path, sub)
                copy.start()
                sends.append(copy)
    for copy in copies:
        copy.wait()
    yield
    zero = (0,) * depth
    stored = []
    for level in range(depth):
        last = level == depth - 1
        if last:
            for load in loads:
                load.wait()
        for path in suffixes(depth - 1 - level):
            for sub in range(subs):
                for tree in trees:
                    reduce_copy(tree, level, path, sub).wait_recv()
                    slot = tree.slot(level, path)
                    first = tree.own_rows((0,) + path if level == 0 else zero, sub, sub_rows)

                    def strip(step, tree=tree, slot=slot, first=first, path=path, sub=sub, level=level, last=last):
                        line = sub * sub_rows + step * STRIP
                        here = pl.ds(pl.multiple_of(line, STRIP), STRIP)
                        if level == 0:
                            mine = own[tree.number, pl.ds(pl.multiple_of(first + step * STRIP, STRIP), STRIP), :]
                        else:
                            mine = slots[tree.number, tree.slot(level - 1, (0,) + path), here, :]
                        total = mine.astype(jnp.float32) + slots[tree.number, slot, here, :].astype(jnp.float32)
                        if last:
                            outbuf[tree.number, here, :] = finish(
                                total, tree.number, here, pl.ds(pl.multiple_of(tree.number * unit + line, STRIP), STRIP)
                            )
                        else:
                            slots[tree.number, slot, here, :] = total.astype(slots.dtype)

                    pl.loop(0, sub_rows // STRIP)(strip)
                    if last:
                        keep = pltpu.make_async_copy(
                            outbuf.at[tree.number, pl.ds(sub * sub_rows, sub_rows), :],
                            out.at[tree.rows(zero, sub, sub_rows), :],
                            local_sem.at[2 + tree.number * subs + sub],
                        )
                        keep.start()
                        stored.append(keep)
                        for back in reversed(range(depth)):
                            copy = gather_copy(tree, back, zero, sub)
                            copy.start()
                            sends.append(copy)
                    elif path[0] == 1:
                        copy = reduce_copy(tree, level + 1, path[1:], sub)
                        copy.start()
                        sends.append(copy)
                yield
    for level in reversed(range(depth)):
        for path in suffixes(depth - 1 - level):
            full = (0,) * level + (1,) + path
            sender = (0,) * (level + 1) + path
            for sub in range(subs):
                for tree in trees:
                    gather_copy(tree, level, sender, sub).wait_recv()
                    for back in reversed(range(level)):
                        copy = gather_copy(tree, back, full, sub)
                        copy.start()
                        sends.append(copy)
                yield
    for copy in sends:
        copy.wait_send()
    for copy in stored:
        copy.wait()


def greet(axis, size):
    barrier = pltpu.get_barrier_semaphore()
    me = lax.axis_index(axis)
    for step in range(1, size):
        pl.semaphore_signal(
            barrier, inc=1, device_id={axis: (me + step) % size}, device_id_type=pl.DeviceIdType.MESH
        )
    pl.semaphore_wait(barrier, size - 1)


def run_together(streams):
    waiting = list(streams)
    while waiting:
        left = []
        for one in waiting:
            try:
                next(one)
                left.append(one)
            except StopIteration:
                pass
        waiting = left


def stream_scratch(size, rows, width):
    half = rows // 2
    unit = half // size
    subs = pieces(unit)
    count = 2 * 2 * (size - 1) * subs
    return [
        pltpu.VMEM((2, half // 2, width), jnp.bfloat16),
        pltpu.VMEM((2, size - 1, unit, width), jnp.bfloat16),
        pltpu.VMEM((2, unit, width), jnp.bfloat16),
        pltpu.SemaphoreType.DMA((2 + 2 * subs,)),
        pltpu.SemaphoreType.DMA((count,)),
        pltpu.SemaphoreType.DMA((count,)),
    ]


def load_rows(axis, size, rows, source, target, sems):
    copies = []
    for number in (0, 1):
        tree = Tree(axis, size, number, rows)
        unit = tree.unit
        copies.append(
            pltpu.make_async_copy(
                source.at[tree.rows((0,) * tree.depth, 0, unit), :], target.at[number], sems.at[number]
            )
        )
    for copy in copies:
        copy.start()
    return copies


def moments(values):
    center = values - jnp.mean(values, axis=-1, keepdims=True)
    scale = lax.rsqrt(jnp.mean(center * center, axis=-1, keepdims=True) + EPS)
    return center * scale, scale


def norm_back(grad, gain, scaled, scale):
    inner = grad * gain
    return scale * (
        inner
        - jnp.mean(inner, axis=-1, keepdims=True)
        - scaled * jnp.mean(inner * scaled, axis=-1, keepdims=True)
    )


def fold(values):
    return values[:8] + values[8:]


HBM = pl.BlockSpec(memory_space=pl.ANY)
VMEM = pl.BlockSpec(memory_space=pltpu.VMEM)


def middle_kernel(size, rows, width, part, tokens, pbias, gain, shift, hidden, mid, own, slots, outbuf, local_sem, send_sem, recv_sem, tok, load_sem):
    greet("tensor", size)
    loads = load_rows("tensor", size, rows, tokens, tok, load_sem)

    def finish(total, number, here, line):
        value = tok[number, here, :].astype(jnp.float32) + total + pbias[...]
        mid[line, :] = value
        scaled, _ = moments(value)
        return (scaled * gain[...] + shift[...]).astype(jnp.bfloat16)

    run_together(
        [stream("tensor", size, (rows, width), part, hidden, own, slots, outbuf, local_sem, send_sem, recv_sem, finish, loads)]
    )


def reduce_middle(size, part, tokens, pbias, gain, shift):
    rows, width = part.shape
    unit = rows // 2 // size
    return pl.pallas_call(
        functools.partial(middle_kernel, size, rows, width),
        out_shape=(
            jax.ShapeDtypeStruct((rows, width), jnp.bfloat16),
            jax.ShapeDtypeStruct((2 * unit, width), jnp.float32),
        ),
        in_specs=[HBM, HBM, VMEM, VMEM, VMEM],
        out_specs=(HBM, VMEM),
        scratch_shapes=stream_scratch(size, rows, width)
        + [pltpu.VMEM((2, unit, width), jnp.bfloat16), pltpu.SemaphoreType.DMA((2,))],
        compiler_params=pltpu.CompilerParams(collective_id=1, has_side_effects=True),
        name="reduce_middle",
    )(part, tokens, pbias, gain, shift)


def back_kernel(size, rows, width, part, d_out, mid, gain, low, dmid, sums, own, slots, outbuf, local_sem, send_sem, recv_sem, dout, load_sem):
    greet("tensor", size)
    loads = load_rows("tensor", size, rows, d_out, dout, load_sem)
    sums[...] = jnp.zeros_like(sums)

    def finish(total, number, here, line):
        scaled, scale = moments(mid[line, :])
        direct = dout[number, here, :].astype(jnp.float32)
        value = direct + norm_back(total, gain[...], scaled, scale)
        dmid[line, :] = value
        sums[0] += fold(total * scaled)
        sums[1] += fold(total)
        sums[2] += fold(value)
        sums[3] += fold(direct)
        return value.astype(jnp.bfloat16)

    run_together(
        [stream("tensor", size, (rows, width), part, low, own, slots, outbuf, local_sem, send_sem, recv_sem, finish, loads)]
    )


def reduce_back(size, part, d_out, mid, gain):
    rows, width = part.shape
    unit = rows // 2 // size
    return pl.pallas_call(
        functools.partial(back_kernel, size, rows, width),
        out_shape=(
            jax.ShapeDtypeStruct((rows, width), jnp.bfloat16),
            jax.ShapeDtypeStruct((2 * unit, width), jnp.float32),
            jax.ShapeDtypeStruct((4, 8, width), jnp.float32),
        ),
        in_specs=[HBM, HBM, VMEM, VMEM],
        out_specs=(HBM, VMEM, VMEM),
        scratch_shapes=stream_scratch(size, rows, width)
        + [pltpu.VMEM((2, unit, width), jnp.bfloat16), pltpu.SemaphoreType.DMA((2,))],
        compiler_params=pltpu.CompilerParams(collective_id=2, has_side_effects=True),
        name="reduce_back",
    )(part, d_out, mid, gain)


def remote_copy(axis, target, src, dst, send_sem, recv_sem):
    return pltpu.make_async_remote_copy(
        src_ref=src,
        dst_ref=dst,
        send_sem=send_sem,
        recv_sem=recv_sem,
        device_id={axis: target},
        device_id_type=pl.DeviceIdType.MESH,
    )


CHUNK = 64
LAG = 3
CORE_SEND, CORE_RECV, UP_SEND, LEFT_RECV, RIGHT_RECV, BACK_LEFT, BACK_RIGHT, BACK_RECV, TWIN_SEND, TWIN_RECV, KEEP, LOAD = range(12)


def chain_scratch(shape):
    half = shape[0] // 2
    return [pltpu.VMEM((half, shape[1]), jnp.bfloat16)] * 4 + [pltpu.SemaphoreType.DMA((12, half // CHUNK))]


def chain(devices, shape, array, out, own, twin, left, right, sems):
    half = shape[0] // 2
    count = half // CHUNK
    length = devices // 2
    me = lax.axis_index("dp")
    core, place = me % 2, me // 2
    other = me + 1 - 2 * core

    def at(ref, chunk):
        return ref.at[pl.ds(pl.multiple_of(chunk * CHUNK, CHUNK), CHUNK), :]

    def part(ref, side, chunk):
        return ref.at[pl.ds(pl.multiple_of(side * half + chunk * CHUNK, CHUNK), CHUNK), :]

    def root(chunk):
        return length // 2 - 1 + chunk % 2

    def core_copy(chunk):
        return remote_copy("dp", other, part(array, 1 - core, chunk), at(twin, chunk), sems.at[CORE_SEND, chunk], sems.at[CORE_RECV, chunk])

    def load(chunk):
        return pltpu.make_async_copy(part(array, core, chunk), at(own, chunk), sems.at[LOAD, chunk])

    def to_right(chunk):
        return remote_copy("dp", me + 2, at(own, chunk), at(left, chunk), sems.at[UP_SEND, chunk], sems.at[LEFT_RECV, chunk])

    def to_left(chunk):
        return remote_copy("dp", me - 2, at(own, chunk), at(right, chunk), sems.at[UP_SEND, chunk], sems.at[RIGHT_RECV, chunk])

    def spread(chunk, src, step, send):
        return remote_copy("dp", me + step, src, part(out, core, chunk), sems.at[send, chunk], sems.at[BACK_RECV, chunk])

    def twin_copy(chunk, src):
        return remote_copy("dp", other, src, part(out, core, chunk), sems.at[TWIN_SEND, chunk], sems.at[TWIN_RECV, chunk])

    def twin_arrival(chunk):
        there = part(out, 1 - core, chunk)
        return remote_copy("dp", other, there, there, sems.at[TWIN_SEND, chunk], sems.at[TWIN_RECV, chunk])

    def keep(chunk):
        return pltpu.make_async_copy(at(own, chunk), part(out, core, chunk), sems.at[KEEP, chunk])

    def add(chunk, terms):
        def strip(step):
            line = pl.ds(pl.multiple_of(chunk * CHUNK + step * STRIP, STRIP), STRIP)
            total = own[line, :].astype(jnp.float32)
            for term in terms:
                total = total + term[line, :].astype(jnp.float32)
            own[line, :] = total.astype(own.dtype)

        pl.loop(0, CHUNK // STRIP)(strip)

    def gather_up(chunk):
        core_copy(chunk).wait_recv()
        load(chunk).wait()
        goal = root(chunk)
        has_left = (place > 0) & (place <= goal)
        has_right = (place < length - 1) & (place >= goal)

        @pl.when(has_left)
        def _():
            to_right(chunk).wait_recv()

        @pl.when(has_right)
        def _():
            to_left(chunk).wait_recv()

        @pl.when(has_left & has_right)
        def _():
            add(chunk, [twin, left, right])

        @pl.when(has_left & ~has_right)
        def _():
            add(chunk, [twin, left])

        @pl.when(has_right & ~has_left)
        def _():
            add(chunk, [twin, right])

        @pl.when(~has_right & ~has_left)
        def _():
            add(chunk, [twin])

        @pl.when(place < goal)
        def _():
            to_right(chunk).start()

        @pl.when(place > goal)
        def _():
            to_left(chunk).start()

        @pl.when(place == goal)
        def _():
            @pl.when(place > 0)
            def _():
                spread(chunk, at(own, chunk), -2, BACK_LEFT).start()

            @pl.when(place < length - 1)
            def _():
                spread(chunk, at(own, chunk), 2, BACK_RIGHT).start()

            twin_copy(chunk, at(own, chunk)).start()
            keep(chunk).start()

    def hand_back(chunk):
        goal = root(chunk)
        here = part(out, core, chunk)

        @pl.when(place < goal)
        def _():
            spread(chunk, here, 2, BACK_RIGHT).wait_recv()

            @pl.when(place > 0)
            def _():
                spread(chunk, here, -2, BACK_LEFT).start()

            twin_copy(chunk, here).start()

        @pl.when(place > goal)
        def _():
            spread(chunk, here, -2, BACK_LEFT).wait_recv()

            @pl.when(place < length - 1)
            def _():
                spread(chunk, here, 2, BACK_RIGHT).start()

            twin_copy(chunk, here).start()

    def finish(chunk):
        goal = root(chunk)
        here = part(out, core, chunk)
        core_copy(chunk).wait_send()
        twin_arrival(chunk).wait_recv()
        twin_copy(chunk, here).wait_send()

        @pl.when(place < goal)
        def _():
            to_right(chunk).wait_send()

        @pl.when(place > goal)
        def _():
            to_left(chunk).wait_send()

        @pl.when((place <= goal) & (place > 0))
        def _():
            spread(chunk, here, -2, BACK_LEFT).wait_send()

        @pl.when((place >= goal) & (place < length - 1))
        def _():
            spread(chunk, here, 2, BACK_RIGHT).wait_send()

        @pl.when(place == goal)
        def _():
            keep(chunk).wait()

    @pl.loop(0, count)
    def _(chunk):
        core_copy(chunk).start()
        load(chunk).start()

    yield
    groups = count // 2
    for step in range(groups + LAG):
        if step < groups:

            @pl.loop(2 * step, 2 * step + 2)
            def _(chunk):
                gather_up(chunk)

        if step >= LAG:

            @pl.loop(2 * (step - LAG), 2 * (step - LAG) + 2)
            def _(chunk):
                hand_back(chunk)

        yield

    @pl.loop(0, count)
    def _(chunk):
        finish(chunk)


def small_scratch(size, devices, width):
    return [
        pltpu.VMEM((size, 8, width), jnp.float32),
        pltpu.VMEM((devices, 16, width), jnp.float32),
        pltpu.SemaphoreType.DMA((2, size)),
        pltpu.SemaphoreType.DMA((2, devices)),
    ]


def small_sum(size, devices, given, sums, out, near, far, near_sem, far_sem):
    def exchange(axis, members, slots, sem):
        me = lax.axis_index(axis)
        copies = []
        for step in range(1, members):
            target = (me + step) % members
            copy = remote_copy(axis, target, slots.at[me], slots.at[me], sem.at[0, target], sem.at[1, me])
            copy.start()
            copies.append(copy)
        for step in range(1, members):
            source = (me + step) % members
            remote_copy(axis, source, slots.at[source], slots.at[source], sem.at[0, source], sem.at[1, source]).wait_recv()
        for copy in copies:
            copy.wait_send()

    mine = given[0:8, :]
    row = lax.broadcasted_iota(jnp.int32, mine.shape, 0)
    mine = jnp.where(row == 0, jnp.sum(sums[0], axis=0, keepdims=True), mine)
    mine = jnp.where(row == 1, jnp.sum(sums[1], axis=0, keepdims=True), mine)
    near[lax.axis_index("tensor")] = mine
    exchange("tensor", size, near, near_sem)
    total = near[0]
    for member in range(1, size):
        total = total + near[member]
    me = lax.axis_index("dp")
    far[me, 0:8, :] = total
    far[me, 8:16, :] = given[8:16, :]
    exchange("dp", devices, far, far_sem)
    total = far[0]
    for member in range(1, devices):
        total = total + far[member]
    out[...] = total


def one_after_another(*parts):
    for part in parts:
        yield from part


def greet_all(sizes):
    barrier = pltpu.get_barrier_semaphore()
    total = 0
    for axis, size in sizes:
        me = lax.axis_index(axis)
        for step in range(1, size):
            pl.semaphore_signal(
                barrier, inc=1, device_id={axis: (me + step) % size}, device_id_type=pl.DeviceIdType.MESH
            )
        total += size - 1
    pl.semaphore_wait(barrier, total)


def later(call):
    call()
    yield


def last_kernel(size, devices, shapes, mlp, part, kv, tokens, mid, dmid, dbias, gain, small, *rest):
    wide, kv_shape, summed = shapes[0], shapes[1], shapes[2:]
    count = len(summed)
    arrays, rest = rest[:count], rest[count:]
    result, grad, kv_sum, small_out, rest = *rest[:4], rest[4:]
    outs, rest = rest[:count], rest[count:]
    kv_out, rest = rest[0], rest[1:]
    first, second, third, rest = rest[:6], rest[6:12], rest[12:18], rest[18:]
    tok, load_sem, sums, rest = *rest[:3], rest[3:]
    near, rest = rest[:4], rest[4:]
    chains = [rest[5 * place : 5 * place + 5] for place in range(count + 1)]
    greet_all((("tensor", size), ("dp", devices)))
    loads = load_rows("tensor", size, wide[0], tokens, tok, load_sem)
    sums[...] = jnp.zeros_like(sums)

    def finish_result(total, number, here, line):
        return (mid[line, :] + total + dbias[...]).astype(jnp.bfloat16)

    def finish_grad(total, number, here, line):
        scaled, scale = moments(tok[number, here, :].astype(jnp.float32))
        sums[0] += fold(total * scaled)
        sums[1] += fold(total)
        return (dmid[line, :] + norm_back(total, gain[...], scaled, scale)).astype(jnp.bfloat16)

    def finish_kv(total, number, here, line):
        return total.astype(jnp.bfloat16)

    def small_part():
        small_sum(size, devices, small, sums, small_out, *near)

    run_together(
        [
            one_after_another(
                *(
                    chain(devices, shape, array, out, *scratch)
                    for shape, array, out, scratch in zip(summed, arrays, outs, chains)
                )
            ),
            one_after_another(
                stream("tensor", size, kv_shape, kv, kv_out, *third, finish_kv),
                chain(devices, kv_shape, kv_out, kv_sum, *chains[-1]),
            ),
            one_after_another(
                stream("tensor", size, wide, part, grad, *second, finish_grad, loads),
                later(small_part),
            ),
            stream("tensor", size, wide, mlp, result, *first, finish_result),
        ]
    )


def reduce_last(size, devices, mlp, part, kv, tokens, mid, dmid, dbias, gain, small, arrays):
    rows, width = part.shape
    unit = rows // 2 // size
    shapes = (part.shape, kv.shape) + tuple(array.shape for array in arrays)
    low = jnp.bfloat16
    outs = pl.pallas_call(
        functools.partial(last_kernel, size, devices, shapes),
        out_shape=(
            jax.ShapeDtypeStruct((rows, width), low),
            jax.ShapeDtypeStruct((rows, width), low),
            jax.ShapeDtypeStruct(kv.shape, low),
            jax.ShapeDtypeStruct(small.shape, jnp.float32),
            *(jax.ShapeDtypeStruct(array.shape, low) for array in arrays),
            jax.ShapeDtypeStruct(kv.shape, low),
        ),
        in_specs=[HBM] * 4 + [VMEM] * 5 + [HBM] * len(arrays),
        out_specs=(HBM, HBM, HBM, VMEM) + (HBM,) * len(arrays) + (HBM,),
        scratch_shapes=stream_scratch(size, rows, width) * 2
        + stream_scratch(size, kv.shape[0], width)
        + [
            pltpu.VMEM((2, unit, width), low),
            pltpu.SemaphoreType.DMA((2,)),
            pltpu.VMEM((2, 8, width), jnp.float32),
        ]
        + small_scratch(size, devices, width)
        + [one for shape in shapes[2:] + (kv.shape,) for one in chain_scratch(shape)],
        compiler_params=pltpu.CompilerParams(
            collective_id=3, has_side_effects=True, vmem_limit_bytes=60 * 1024 * 1024
        ),
        name="reduce_last",
    )(mlp, part, kv, tokens, mid, dmid, dbias, gain, small, *arrays)
    return outs[:4], outs[4 : 4 + len(arrays)]


def layer_norm(values, gain, shift):
    center = values - jnp.mean(values, axis=-1, keepdims=True)
    scaled = center * lax.rsqrt(jnp.mean(center * center, axis=-1, keepdims=True) + 1e-05)
    return scaled * gain + shift


def gelu_tanh(values):
    return (
        0.5
        * values
        * (1.0 + jnp.tanh(0.7978845608028654 * (values + 0.044715 * values * values * values)))
    )


def contract_rows(left, right):
    return lax.dot_general(
        left, right, (((0,), (0,)), ((), ())), preferred_element_type=jnp.float32
    )


def contract_cols(left, right):
    return lax.dot_general(
        left, right, (((1,), (1,)), ((), ())), preferred_element_type=jnp.float32
    )


def block_scores(query_block, key_rows, offset, length):
    scale = query_block.shape[2] ** (-0.5)
    scores = (
        jnp.einsum("qhd,kd->hqk", query_block, key_rows, preferred_element_type=jnp.float32) * scale
    )
    rows_pos = offset + jnp.arange(query_block.shape[0], dtype=jnp.int32)
    keys_pos = jnp.arange(key_rows.shape[0], dtype=jnp.int32)
    allowed = (keys_pos[None, :] <= rows_pos[:, None]) & (keys_pos[None, :] < length)
    return jnp.where(allowed[None], scores, -1e30)


def attend_forward(queries, key_rows, value_rows, length, block_rows):
    pieces = []
    log_totals = []
    for offset in range(0, queries.shape[0], block_rows):
        query_block = queries[offset : offset + block_rows]
        scores = block_scores(query_block, key_rows, offset, length)
        highest = jnp.max(scores, axis=-1, keepdims=True)
        exponent = jnp.exp(scores - highest)
        normaliser = jnp.sum(exponent, axis=-1, keepdims=True)
        probability = (exponent / normaliser).astype(jnp.bfloat16)
        log_totals.append(highest + jnp.log(normaliser))
        pieces.append(
            jnp.einsum("hqk,kd->qhd", probability, value_rows, preferred_element_type=jnp.float32)
        )
    return (jnp.concatenate(pieces, axis=0), log_totals)


def attend_backward(queries, key_rows, value_rows, length, block_rows, log_totals, grad_heads):
    scale = queries.shape[2] ** (-0.5)
    query_grads = []
    key_grads = jnp.zeros(key_rows.shape, jnp.float32)
    value_grads = jnp.zeros(value_rows.shape, jnp.float32)
    for counter, offset in enumerate(range(0, queries.shape[0], block_rows)):
        query_block = queries[offset : offset + block_rows]
        grad_block = grad_heads[offset : offset + block_rows]
        scores = block_scores(query_block, key_rows, offset, length)
        probability = jnp.exp(scores - log_totals[counter])
        grad_probs = jnp.einsum(
            "qhd,kd->hqk", grad_block, value_rows, preferred_element_type=jnp.float32
        )
        inner = jnp.sum(probability * grad_probs, axis=-1, keepdims=True)
        grad_scores = (probability * (grad_probs - inner)).astype(jnp.bfloat16)
        query_grads.append(
            (
                jnp.einsum("hqk,kd->qhd", grad_scores, key_rows, preferred_element_type=jnp.float32)
                * scale
            ).astype(jnp.bfloat16)
        )
        key_grads = (
            key_grads
            + jnp.einsum(
                "hqk,qhd->kd", grad_scores, query_block, preferred_element_type=jnp.float32
            )
            * scale
        )
        value_grads = value_grads + jnp.einsum(
            "hqk,qhd->kd",
            probability.astype(jnp.bfloat16),
            grad_block,
            preferred_element_type=jnp.float32,
        )
    return (jnp.concatenate(query_grads, axis=0), key_grads, value_grads)


def local(
    size,
    devices,
    tokens,
    lengths,
    norm1_gain,
    norm1_shift,
    query_weight,
    query_bias,
    keyval_weight,
    value_bias,
    proj_weight,
    proj_bias,
    norm2_gain,
    norm2_shift,
    up_weight,
    up_bias,
    down_weight,
    down_bias,
    cotangent,
):
    wide = jnp.float32
    slot_len, width = tokens.shape
    head_dim = keyval_weight.shape[1] // 2
    heads_here = query_weight.shape[1] // head_dim
    block_rows = min(512, slot_len)
    length = lengths[0]

    def row(vector):
        return vector.astype(wide).reshape(1, -1)

    hidden1 = layer_norm(tokens.astype(wide), norm1_gain.astype(wide), norm1_shift.astype(wide)).astype(jnp.bfloat16)
    queries = (
        jnp.dot(hidden1, query_weight, preferred_element_type=wide) + query_bias.astype(wide)
    ).astype(jnp.bfloat16)
    keyval = jnp.dot(hidden1, keyval_weight, preferred_element_type=wide)
    key_rows = keyval[:, :head_dim].astype(jnp.bfloat16)
    value_rows = (keyval[:, head_dim:] + value_bias.astype(wide)).astype(jnp.bfloat16)
    slot_queries = queries.reshape(slot_len, heads_here, head_dim)
    attended, log_totals = attend_forward(slot_queries, key_rows, value_rows, length, block_rows)
    heads_out = attended.reshape(slot_len, heads_here * head_dim).astype(jnp.bfloat16)
    attn_terms = jnp.dot(heads_out, proj_weight, preferred_element_type=wide).astype(jnp.bfloat16)
    hidden2, mid = reduce_middle(size, attn_terms, tokens, row(proj_bias), row(norm2_gain), row(norm2_shift))

    pre_act = jnp.dot(hidden2, up_weight, preferred_element_type=wide) + up_bias.astype(wide)
    activated = gelu_tanh(pre_act).astype(jnp.bfloat16)
    valid = (jnp.arange(slot_len, dtype=jnp.int32) < length)[:, None]
    d_out = jnp.where(valid, cotangent, jnp.zeros_like(cotangent))
    grad_down = contract_rows(activated, d_out).astype(jnp.bfloat16)
    grad_down = lax.psum(grad_down, "dp")
    grad_act = contract_cols(d_out, down_weight).astype(jnp.bfloat16)
    gelu_pull = jax.vjp(gelu_tanh, pre_act)[1]
    grad_pre = gelu_pull(grad_act.astype(wide))[0].astype(jnp.bfloat16)
    back2 = contract_cols(grad_pre, up_weight).astype(jnp.bfloat16)
    middle_low, dmid, sums2 = reduce_back(size, back2, d_out, mid, row(norm2_gain))
    grad_up = contract_rows(hidden2, grad_pre).astype(jnp.bfloat16)
    grad_upbias = jnp.sum(grad_pre.astype(wide), axis=0)
    mlp_terms = jnp.dot(activated, down_weight, preferred_element_type=wide).astype(jnp.bfloat16)

    grad_proj = contract_rows(heads_out, middle_low).astype(jnp.bfloat16)
    grad_heads = contract_cols(middle_low, proj_weight).astype(jnp.bfloat16)
    slot_grads = grad_heads.reshape(slot_len, heads_here, head_dim)
    query_part, key_part, value_part = attend_backward(
        slot_queries, key_rows, value_rows, length, block_rows, log_totals, slot_grads
    )
    grad_queries = query_part.reshape(slot_len, heads_here * head_dim)
    grad_kv_rows = jnp.concatenate([key_part, value_part], axis=1).astype(jnp.bfloat16)
    grad_qbias = jnp.sum(grad_queries.astype(wide), axis=0)
    grad_query = contract_rows(grad_queries, hidden1).astype(jnp.bfloat16)
    grad_keyval = contract_rows(grad_kv_rows, hidden1).astype(jnp.bfloat16)
    grad_vbias = jnp.sum(grad_kv_rows[:, head_dim:].astype(wide), axis=0)
    back1 = (
        contract_cols(grad_queries, query_weight) + contract_cols(grad_kv_rows, keyval_weight)
    ).astype(jnp.bfloat16)

    def padded(vector):
        return jnp.pad(vector, (0, width - vector.shape[0])).reshape(1, width)

    small = jnp.concatenate(
        [
            jnp.zeros((2, width), wide),
            jnp.sum(sums2, axis=1),
            padded(grad_vbias),
            jnp.zeros((1, width), wide),
            padded(grad_qbias),
            padded(grad_upbias),
            jnp.zeros((6, width), wide),
        ]
    )
    (result, grad_tokens, kv_sum, small), (grad_up, grad_proj, grad_query) = reduce_last(
        size,
        devices,
        mlp_terms,
        back1,
        grad_keyval,
        tokens,
        mid,
        dmid,
        row(down_bias),
        row(norm1_gain),
        small,
        (grad_up, grad_proj, grad_query),
    )
    grad_gain1, grad_shift1, grad_gain2, grad_shift2, grad_pbias, grad_dnbias = (
        small[place] for place in range(6)
    )
    grad_vbias = small[6, :head_dim]
    grad_qbias = small[8, : query_bias.shape[0]]
    grad_upbias = small[9, : up_bias.shape[0]]
    return (
        result,
        grad_tokens,
        grad_gain1,
        grad_shift1,
        grad_query.T.astype(wide),
        grad_qbias,
        kv_sum.T.astype(wide),
        grad_vbias,
        grad_proj.astype(wide),
        grad_pbias,
        grad_gain2,
        grad_shift2,
        grad_up.astype(wide),
        grad_upbias,
        grad_down.astype(wide),
        grad_dnbias,
    )


def solution(mesh):
    in_specs = (
        P("dp", None),
        P("dp"),
        P(),
        P(),
        P(None, "tensor"),
        P("tensor"),
        P(),
        P(),
        P("tensor", None),
        P(),
        P(),
        P(),
        P(None, "tensor"),
        P("tensor"),
        P("tensor", None),
        P(),
        P("dp", None),
    )
    out_specs = (
        P("dp", None),
        P("dp", None),
        P(),
        P(),
        P(None, "tensor"),
        P("tensor"),
        P(),
        P(),
        P("tensor", None),
        P(),
        P(),
        P(),
        P(None, "tensor"),
        P("tensor"),
        P("tensor", None),
        P(),
    )
    return jax.shard_map(functools.partial(local, mesh.shape["tensor"], mesh.shape["dp"]), mesh=mesh, in_specs=in_specs, out_specs=out_specs, check_vma=False)
```

```python
import functools

import jax
import jax.numpy as jnp
from jax import lax
from jax.experimental import pallas as pl
from jax.experimental.pallas import tpu as pltpu
from jax.sharding import PartitionSpec as P

STRIP = 16
EPS = 1e-05


def suffixes(count):
    if count == 0:
        return [()]
    rest = [()]
    for _ in range(count - 1):
        rest = [(bit,) + more for bit in (1, 0) for more in rest]
    return [(bit,) + more for bit in (1, 0) for more in rest]


def pieces(unit):
    return 2 if unit % (2 * STRIP) == 0 else 1


def as_number(path):
    total = 0
    for bit in path:
        total = 2 * total + bit
    return total


class Tree:
    def __init__(self, axis, size, number, rows):
        self.axis, self.size = axis, size
        self.depth = size.bit_length() - 1
        self.number = number
        self.half = rows // 2
        self.unit = self.half // size
        order = list(range(self.depth))
        self.order = order if number == 0 else order[::-1]
        me = lax.axis_index(axis)
        self.mine = [(me // (1 << bit)) % 2 for bit in self.order]
        self.partners = [me + (1 - 2 * own) * (1 << bit) for own, bit in zip(self.mine, self.order)]

    def offset(self, path, skip=0):
        start = 0
        for level in range(skip, self.depth):
            side = (self.mine[level] + path[level]) % 2
            start = start + side * (self.half >> (level + 1))
        return start

    def rows(self, path, sub, sub_rows):
        start = self.number * self.half + self.offset(path) + sub * sub_rows
        return pl.ds(pl.multiple_of(start, sub_rows), sub_rows)

    def own_rows(self, path, sub, sub_rows):
        start = self.offset(path, 1) + sub * sub_rows
        return pl.multiple_of(start, sub_rows)

    def slot(self, level, path):
        base = sum(1 << (self.depth - 1 - lower) for lower in range(level))
        return base + as_number(path)


def stream(axis, size, shape, part, out, own, slots, outbuf, local_sem, send_sem, recv_sem, finish, loads=()):
    rows, width = shape
    trees = [Tree(axis, size, number, rows) for number in (0, 1)]
    unit = trees[0].unit
    depth = trees[0].depth
    subs = pieces(unit)
    sub_rows = unit // subs
    sends = []

    def remote(tree, src, dst, kind, index, sub, level):
        place = ((tree.number * 2 + kind) * (size - 1) + index) * subs + sub
        copy = pltpu.make_async_remote_copy(
            src_ref=src,
            dst_ref=dst,
            send_sem=send_sem.at[place],
            recv_sem=recv_sem.at[place],
            device_id={axis: tree.partners[level]},
            device_id_type=pl.DeviceIdType.MESH,
        )
        return copy

    def reduce_copy(tree, level, path, sub):
        slot = tree.slot(level, path)
        if level == 0:
            src = part.at[tree.rows((1,) + path, sub, sub_rows), :]
        else:
            src = slots.at[tree.number, tree.slot(level - 1, (1,) + path), pl.ds(sub * sub_rows, sub_rows), :]
        dst = slots.at[tree.number, slot, pl.ds(sub * sub_rows, sub_rows), :]
        return remote(tree, src, dst, 0, slot, sub, level)

    def gather_copy(tree, level, path, sub):
        there = path[:level] + (1,) + path[level + 1 :]
        where = tree.rows(path, sub, sub_rows)
        if any(path):
            src = out.at[where, :]
        else:
            src = outbuf.at[tree.number, pl.ds(sub * sub_rows, sub_rows), :]
        return remote(tree, src, out.at[where, :], 1, as_number(there) - 1, sub, level)

    copies = []
    for tree in trees:
        start = tree.number * tree.half + tree.mine[0] * (tree.half // 2)
        copies.append(
            pltpu.make_async_copy(
                part.at[pl.ds(pl.multiple_of(start, tree.half // 2), tree.half // 2), :],
                own.at[tree.number],
                local_sem.at[tree.number],
            )
        )
    for copy in copies:
        copy.start()
    for path in suffixes(depth - 1):
        for sub in range(subs):
            for tree in trees:
                copy = reduce_copy(tree, 0, path, sub)
                copy.start()
                sends.append(copy)
    for copy in copies:
        copy.wait()
    yield True
    zero = (0,) * depth
    stored = []
    for level in range(depth):
        last = level == depth - 1
        if last:
            for load in loads:
                load.wait()
        paths = suffixes(depth - 1 - level)
        for path in paths:
            for sub in range(subs):
                for tree in trees:
                    reduce_copy(tree, level, path, sub).wait_recv()
                    slot = tree.slot(level, path)
                    first = tree.own_rows((0,) + path if level == 0 else zero, sub, sub_rows)

                    def strip(step, tree=tree, slot=slot, first=first, path=path, sub=sub, level=level, last=last):
                        line = sub * sub_rows + step * STRIP
                        here = pl.ds(pl.multiple_of(line, STRIP), STRIP)
                        if level == 0:
                            mine = own[tree.number, pl.ds(pl.multiple_of(first + step * STRIP, STRIP), STRIP), :]
                        else:
                            mine = slots[tree.number, tree.slot(level - 1, (0,) + path), here, :]
                        total = mine.astype(jnp.float32) + slots[tree.number, slot, here, :].astype(jnp.float32)
                        if last:
                            outbuf[tree.number, here, :] = finish(
                                total, tree.number, here, pl.ds(pl.multiple_of(tree.number * unit + line, STRIP), STRIP)
                            )
                        else:
                            slots[tree.number, slot, here, :] = total.astype(slots.dtype)

                    pl.loop(0, sub_rows // STRIP)(strip)
                    if last:
                        keep = pltpu.make_async_copy(
                            outbuf.at[tree.number, pl.ds(sub * sub_rows, sub_rows), :],
                            out.at[tree.rows(zero, sub, sub_rows), :],
                            local_sem.at[2 + tree.number * subs + sub],
                        )
                        keep.start()
                        stored.append(keep)
                        for back in reversed(range(depth)):
                            copy = gather_copy(tree, back, zero, sub)
                            copy.start()
                            sends.append(copy)
                    elif path[0] == 1:
                        copy = reduce_copy(tree, level + 1, path[1:], sub)
                        copy.start()
                        sends.append(copy)
                yield path == paths[-1] and sub == subs - 1
    for level in reversed(range(depth)):
        paths = suffixes(depth - 1 - level)
        for path in paths:
            full = (0,) * level + (1,) + path
            sender = (0,) * (level + 1) + path
            for sub in range(subs):
                for tree in trees:
                    gather_copy(tree, level, sender, sub).wait_recv()
                    for back in reversed(range(level)):
                        copy = gather_copy(tree, back, full, sub)
                        copy.start()
                        sends.append(copy)
                yield path == paths[-1] and sub == subs - 1
    for copy in sends:
        copy.wait_send()
    for copy in stored:
        copy.wait()


def greet(axis, size):
    barrier = pltpu.get_barrier_semaphore()
    me = lax.axis_index(axis)
    for step in range(1, size):
        pl.semaphore_signal(
            barrier, inc=1, device_id={axis: (me + step) % size}, device_id_type=pl.DeviceIdType.MESH
        )
    pl.semaphore_wait(barrier, size - 1)


def run_together(streams):
    waiting = list(streams)
    while waiting:
        left = []
        for one in waiting:
            try:
                next(one)
                left.append(one)
            except StopIteration:
                pass
        waiting = left


def stream_scratch(size, rows, width):
    half = rows // 2
    unit = half // size
    subs = pieces(unit)
    count = 2 * 2 * (size - 1) * subs
    return [
        pltpu.VMEM((2, half // 2, width), jnp.bfloat16),
        pltpu.VMEM((2, size - 1, unit, width), jnp.bfloat16),
        pltpu.VMEM((2, unit, width), jnp.bfloat16),
        pltpu.SemaphoreType.DMA((2 + 2 * subs,)),
        pltpu.SemaphoreType.DMA((count,)),
        pltpu.SemaphoreType.DMA((count,)),
    ]


def load_rows(axis, size, rows, source, target, sems):
    copies = []
    for number in (0, 1):
        tree = Tree(axis, size, number, rows)
        unit = tree.unit
        copies.append(
            pltpu.make_async_copy(
                source.at[tree.rows((0,) * tree.depth, 0, unit), :], target.at[number], sems.at[number]
            )
        )
    for copy in copies:
        copy.start()
    return copies


def moments(values):
    center = values - jnp.mean(values, axis=-1, keepdims=True)
    scale = lax.rsqrt(jnp.mean(center * center, axis=-1, keepdims=True) + EPS)
    return center * scale, scale


def norm_back(grad, gain, scaled, scale):
    inner = grad * gain
    return scale * (
        inner
        - jnp.mean(inner, axis=-1, keepdims=True)
        - scaled * jnp.mean(inner * scaled, axis=-1, keepdims=True)
    )


def fold(values):
    return values[:8] + values[8:]


HBM = pl.BlockSpec(memory_space=pl.ANY)
VMEM = pl.BlockSpec(memory_space=pltpu.VMEM)


def middle_kernel(size, rows, width, part, tokens, pbias, gain, shift, hidden, mid, own, slots, outbuf, local_sem, send_sem, recv_sem, tok, load_sem):
    greet("tensor", size)
    loads = load_rows("tensor", size, rows, tokens, tok, load_sem)

    def finish(total, number, here, line):
        value = tok[number, here, :].astype(jnp.float32) + total + pbias[...]
        mid[line, :] = value
        scaled, _ = moments(value)
        return (scaled * gain[...] + shift[...]).astype(jnp.bfloat16)

    run_together(
        [stream("tensor", size, (rows, width), part, hidden, own, slots, outbuf, local_sem, send_sem, recv_sem, finish, loads)]
    )


def reduce_middle(size, part, tokens, pbias, gain, shift):
    rows, width = part.shape
    unit = rows // 2 // size
    return pl.pallas_call(
        functools.partial(middle_kernel, size, rows, width),
        out_shape=(
            jax.ShapeDtypeStruct((rows, width), jnp.bfloat16),
            jax.ShapeDtypeStruct((2 * unit, width), jnp.float32),
        ),
        in_specs=[HBM, HBM, VMEM, VMEM, VMEM],
        out_specs=(HBM, VMEM),
        scratch_shapes=stream_scratch(size, rows, width)
        + [pltpu.VMEM((2, unit, width), jnp.bfloat16), pltpu.SemaphoreType.DMA((2,))],
        compiler_params=pltpu.CompilerParams(collective_id=1, has_side_effects=True),
        name="reduce_middle",
    )(part, tokens, pbias, gain, shift)


def back_kernel(size, rows, width, part, d_out, mid, gain, low, dmid, sums, own, slots, outbuf, local_sem, send_sem, recv_sem, dout, load_sem):
    greet("tensor", size)
    loads = load_rows("tensor", size, rows, d_out, dout, load_sem)
    sums[...] = jnp.zeros_like(sums)

    def finish(total, number, here, line):
        scaled, scale = moments(mid[line, :])
        direct = dout[number, here, :].astype(jnp.float32)
        value = direct + norm_back(total, gain[...], scaled, scale)
        dmid[line, :] = value
        sums[0] += fold(total * scaled)
        sums[1] += fold(total)
        sums[2] += fold(value)
        sums[3] += fold(direct)
        return value.astype(jnp.bfloat16)

    run_together(
        [stream("tensor", size, (rows, width), part, low, own, slots, outbuf, local_sem, send_sem, recv_sem, finish, loads)]
    )


def reduce_back(size, part, d_out, mid, gain):
    rows, width = part.shape
    unit = rows // 2 // size
    return pl.pallas_call(
        functools.partial(back_kernel, size, rows, width),
        out_shape=(
            jax.ShapeDtypeStruct((rows, width), jnp.bfloat16),
            jax.ShapeDtypeStruct((2 * unit, width), jnp.float32),
            jax.ShapeDtypeStruct((4, 8, width), jnp.float32),
        ),
        in_specs=[HBM, HBM, VMEM, VMEM],
        out_specs=(HBM, VMEM, VMEM),
        scratch_shapes=stream_scratch(size, rows, width)
        + [pltpu.VMEM((2, unit, width), jnp.bfloat16), pltpu.SemaphoreType.DMA((2,))],
        compiler_params=pltpu.CompilerParams(collective_id=2, has_side_effects=True),
        name="reduce_back",
    )(part, d_out, mid, gain)


def remote_copy(axis, target, src, dst, send_sem, recv_sem):
    return pltpu.make_async_remote_copy(
        src_ref=src,
        dst_ref=dst,
        send_sem=send_sem,
        recv_sem=recv_sem,
        device_id={axis: target},
        device_id_type=pl.DeviceIdType.MESH,
    )


CHUNK = 32
SKEW = 1
CORE_SEND, CORE_RECV, UP_SEND, LEFT_RECV, RIGHT_RECV, BACK_LEFT, BACK_RIGHT, BACK_RECV, TWIN_SEND, TWIN_RECV, KEEP, LOAD = range(12)


def chain_scratch(rows, width):
    half = rows // 2
    return [pltpu.VMEM((half, width), jnp.bfloat16)] * 4 + [pltpu.SemaphoreType.DMA((12, half // CHUNK))]


def chain(devices, sources, out, own, twin, left, right, sems):
    length = devices // 2
    me = lax.axis_index("dp")
    core, place = me % 2, me // 2
    other = me + 1 - 2 * core
    deepest = length // 2

    def at(ref, chunk):
        return ref.at[pl.ds(pl.multiple_of(chunk * CHUNK, CHUNK), CHUNK), :]

    def part(ref, side, chunk):
        return ref.at[pl.ds(pl.multiple_of((2 * chunk + side) * CHUNK, CHUNK), CHUNK), :]

    def core_copy(source, chunk, first):
        return remote_copy("dp", other, part(source, 1 - core, chunk - first), at(twin, chunk), sems.at[CORE_SEND, chunk], sems.at[CORE_RECV, chunk])

    def load(source, chunk, first):
        return pltpu.make_async_copy(part(source, core, chunk - first), at(own, chunk), sems.at[LOAD, chunk])

    def to_right(chunk):
        return remote_copy("dp", me + 2, at(own, chunk), at(left, chunk), sems.at[UP_SEND, chunk], sems.at[LEFT_RECV, chunk])

    def to_left(chunk):
        return remote_copy("dp", me - 2, at(own, chunk), at(right, chunk), sems.at[UP_SEND, chunk], sems.at[RIGHT_RECV, chunk])

    def spread(chunk, src, step, send):
        return remote_copy("dp", me + step, src, part(out, core, chunk), sems.at[send, chunk], sems.at[BACK_RECV, chunk])

    def twin_copy(chunk, src):
        return remote_copy("dp", other, src, part(out, core, chunk), sems.at[TWIN_SEND, chunk], sems.at[TWIN_RECV, chunk])

    def twin_arrival(chunk):
        there = part(out, 1 - core, chunk)
        return remote_copy("dp", other, there, there, sems.at[TWIN_SEND, chunk], sems.at[TWIN_RECV, chunk])

    def keep(chunk):
        return pltpu.make_async_copy(at(own, chunk), part(out, core, chunk), sems.at[KEEP, chunk])

    def add(chunk, terms):
        def strip(step):
            line = pl.ds(pl.multiple_of(chunk * CHUNK + step * STRIP, STRIP), STRIP)
            total = own[line, :].astype(jnp.float32)
            for term in terms:
                total = total + term[line, :].astype(jnp.float32)
            own[line, :] = total.astype(own.dtype)

        pl.loop(0, CHUNK // STRIP)(strip)

    def gather_up(chunk, goal):
        core_copy(out, chunk, 0).wait_recv()
        load(out, chunk, 0).wait()
        has_left = (place > 0) & (place <= goal)
        has_right = (place < length - 1) & (place >= goal)

        @pl.when(~has_right & ~has_left)
        def _():
            add(chunk, [twin])

        @pl.when(has_left & ~has_right)
        def _():
            to_right(chunk).wait_recv()
            add(chunk, [twin, left])

        @pl.when(has_right & ~has_left)
        def _():
            to_left(chunk).wait_recv()
            add(chunk, [twin, right])

        @pl.when(has_left & has_right)
        def _():
            to_right(chunk).wait_recv()
            to_left(chunk).wait_recv()
            add(chunk, [twin, left, right])

        @pl.when(place < goal)
        def _():
            to_right(chunk).start()

        @pl.when(place > goal)
        def _():
            to_left(chunk).start()

        @pl.when(place == goal)
        def _():
            @pl.when(place > 0)
            def _():
                spread(chunk, at(own, chunk), -2, BACK_LEFT).start()

            @pl.when(place < length - 1)
            def _():
                spread(chunk, at(own, chunk), 2, BACK_RIGHT).start()

            twin_copy(chunk, at(own, chunk)).start()
            keep(chunk).start()

    def hand_back(chunk, goal):
        here = part(out, core, chunk)

        @pl.when(place < goal)
        def _():
            spread(chunk, here, 2, BACK_RIGHT).wait_recv()

            @pl.when(place > 0)
            def _():
                spread(chunk, here, -2, BACK_LEFT).start()

            twin_copy(chunk, here).start()

        @pl.when(place > goal)
        def _():
            spread(chunk, here, -2, BACK_LEFT).wait_recv()

            @pl.when(place < length - 1)
            def _():
                spread(chunk, here, 2, BACK_RIGHT).start()

            twin_copy(chunk, here).start()

    def finish(chunk, goal):
        here = part(out, core, chunk)
        core_copy(out, chunk, 0).wait_send()
        twin_arrival(chunk).wait_recv()
        twin_copy(chunk, here).wait_send()

        @pl.when(place < goal)
        def _():
            to_right(chunk).wait_send()

        @pl.when(place > goal)
        def _():
            to_left(chunk).wait_send()

        @pl.when((place <= goal) & (place > 0))
        def _():
            spread(chunk, here, -2, BACK_LEFT).wait_send()

        @pl.when((place >= goal) & (place < length - 1))
        def _():
            spread(chunk, here, 2, BACK_RIGHT).wait_send()

        @pl.when(place == goal)
        def _():
            keep(chunk).wait()

    def open_source(source, first, count):
        @pl.loop(first, first + count)
        def _(chunk):
            core_copy(source, chunk, first).start()
            load(source, chunk, first).start()

    late = []
    first = 0
    for source, rows, before in sources:
        count = rows // 2 // CHUNK
        if before is None:
            open_source(source, first, count)
        else:
            late.append((source, first, count, before))
        first += count
    pairs = first // 2
    yield
    for step in range(pairs + SKEW * 2 * deepest):
        for source, begin, count, before in late:
            if step == max(0, begin // 2 - 2):
                for _ in before:
                    pass
                open_source(source, begin, count)
        for parity in (0, 1):
            goal = deepest - 1 + parity
            below = (place < goal).astype(jnp.int32)
            above = (place > goal).astype(jnp.int32)
            level = below * place + above * (length - 1 - place) + (1 - below - above) * deepest
            pair = step - SKEW * level

            @pl.when((pair >= 0) & (pair < pairs))
            def _(parity=parity, goal=goal, pair=pair):
                gather_up(2 * pair + parity, goal)

            away = below * (goal - place) + above * (place - goal)
            pair_back = step - SKEW * (deepest + away)

            @pl.when((away > 0) & (pair_back >= 0) & (pair_back < pairs))
            def _(parity=parity, goal=goal, pair_back=pair_back):
                hand_back(2 * pair_back + parity, goal)

        yield

    @pl.loop(0, pairs)
    def _(pair):
        finish(2 * pair, deepest - 1)
        finish(2 * pair + 1, deepest)


def small_scratch(size, devices, width):
    return [
        pltpu.VMEM((size, 8, width), jnp.float32),
        pltpu.VMEM((devices, 16, width), jnp.float32),
        pltpu.SemaphoreType.DMA((2, size)),
        pltpu.SemaphoreType.DMA((2, devices)),
    ]


def small_sum(size, devices, turns, given, sums, out, near, far, near_sem, far_sem):
    def send(axis, members, slots, sem):
        me = lax.axis_index(axis)
        copies = []
        for step in range(1, members):
            target = (me + step) % members
            copy = remote_copy(axis, target, slots.at[me], slots.at[me], sem.at[0, target], sem.at[1, me])
            copy.start()
            copies.append(copy)
        return copies

    def receive(axis, members, slots, sem, copies):
        me = lax.axis_index(axis)
        for step in range(1, members):
            source = (me + step) % members
            remote_copy(axis, source, slots.at[source], slots.at[source], sem.at[0, source], sem.at[1, source]).wait_recv()
        for copy in copies:
            copy.wait_send()

    for _ in range(turns):
        yield True
    mine = given[0:8, :]
    row = lax.broadcasted_iota(jnp.int32, mine.shape, 0)
    mine = jnp.where(row == 0, jnp.sum(sums[0], axis=0, keepdims=True), mine)
    mine = jnp.where(row == 1, jnp.sum(sums[1], axis=0, keepdims=True), mine)
    near[lax.axis_index("tensor")] = mine
    copies = send("tensor", size, near, near_sem)
    yield True
    receive("tensor", size, near, near_sem, copies)
    total = near[0]
    for member in range(1, size):
        total = total + near[member]
    me = lax.axis_index("dp")
    far[me, 0:8, :] = total
    far[me, 8:16, :] = given[8:16, :]
    copies = send("dp", devices, far, far_sem)
    yield False
    yield False
    receive("dp", devices, far, far_sem, copies)
    total = far[0]
    for member in range(1, devices):
        total = total + far[member]
    out[...] = total


def in_turns(*parts):
    waiting = list(parts)
    while waiting:
        left = []
        for one, quiet in waiting:
            ended = False
            try:
                while not ended:
                    ended = next(one)
                    if not quiet:
                        yield
                left.append((one, quiet))
            except StopIteration:
                pass
        waiting = left


def greet_all(sizes):
    barrier = pltpu.get_barrier_semaphore()
    total = 0
    for axis, size in sizes:
        me = lax.axis_index(axis)
        for step in range(1, size):
            pl.semaphore_signal(
                barrier, inc=1, device_id={axis: (me + step) % size}, device_id_type=pl.DeviceIdType.MESH
            )
        total += size - 1
    pl.semaphore_wait(barrier, total)


def last_kernel(size, devices, shapes, mlp, part, kv, tokens, mid, dmid, dbias, gain, small, *rest):
    wide, kv_shape, summed = shapes[0], shapes[1], shapes[2:]
    arrays, rest = rest[: len(summed)], rest[len(summed) :]
    result, grad, total, small_out, kv_out, rest = *rest[:5], rest[5:]
    first, second, third, rest = rest[:6], rest[6:12], rest[12:18], rest[18:]
    tok, load_sem, sums, rest = *rest[:3], rest[3:]
    greet_all((("tensor", size), ("dp", devices)))
    loads = load_rows("tensor", size, wide[0], tokens, tok, load_sem)
    sums[...] = jnp.zeros_like(sums)

    def finish_result(total, number, here, line):
        return (mid[line, :] + total + dbias[...]).astype(jnp.bfloat16)

    def finish_grad(total, number, here, line):
        scaled, scale = moments(tok[number, here, :].astype(jnp.float32))
        sums[0] += fold(total * scaled)
        sums[1] += fold(total)
        return (dmid[line, :] + norm_back(total, gain[...], scaled, scale)).astype(jnp.bfloat16)

    def finish_kv(total, number, here, line):
        return total.astype(jnp.bfloat16)

    kv_stream = stream("tensor", size, kv_shape, kv, kv_out, *third, finish_kv)
    sources = [(array, shape[0], None) for array, shape in zip(arrays, summed)]
    sources.append((kv_out, kv_shape[0], kv_stream))
    run_together(
        [
            in_turns(
                (kv_stream, True),
                (stream("tensor", size, wide, part, grad, *second, finish_grad, loads), False),
                (stream("tensor", size, wide, mlp, result, *first, finish_result), False),
                (small_sum(size, devices, size.bit_length() - 1, small, sums, small_out, *rest[:4]), False),
            ),
            chain(devices, sources, total, *rest[4:]),
        ]
    )


def reduce_last(size, devices, mlp, part, kv, tokens, mid, dmid, dbias, gain, small, arrays):
    rows, width = part.shape
    unit = rows // 2 // size
    shapes = (part.shape, kv.shape) + tuple(array.shape for array in arrays)
    lines = sum(shape[0] for shape in shapes[1:])
    low = jnp.bfloat16
    return pl.pallas_call(
        functools.partial(last_kernel, size, devices, shapes),
        out_shape=(
            jax.ShapeDtypeStruct((rows, width), low),
            jax.ShapeDtypeStruct((rows, width), low),
            jax.ShapeDtypeStruct((lines, width), low),
            jax.ShapeDtypeStruct(small.shape, jnp.float32),
            jax.ShapeDtypeStruct(kv.shape, low),
        ),
        in_specs=[HBM] * 4 + [VMEM] * 5 + [HBM] * len(arrays),
        out_specs=(HBM, HBM, HBM, VMEM, HBM),
        scratch_shapes=stream_scratch(size, rows, width) * 2
        + stream_scratch(size, kv.shape[0], width)
        + [
            pltpu.VMEM((2, unit, width), low),
            pltpu.SemaphoreType.DMA((2,)),
            pltpu.VMEM((2, 8, width), jnp.float32),
        ]
        + small_scratch(size, devices, width)
        + chain_scratch(lines, width),
        compiler_params=pltpu.CompilerParams(
            collective_id=3, has_side_effects=True, vmem_limit_bytes=60 * 1024 * 1024
        ),
        name="reduce_last",
    )(mlp, part, kv, tokens, mid, dmid, dbias, gain, small, *arrays)[:4]


def layer_norm(values, gain, shift):
    center = values - jnp.mean(values, axis=-1, keepdims=True)
    scaled = center * lax.rsqrt(jnp.mean(center * center, axis=-1, keepdims=True) + 1e-05)
    return scaled * gain + shift


def gelu_tanh(values):
    return (
        0.5
        * values
        * (1.0 + jnp.tanh(0.7978845608028654 * (values + 0.044715 * values * values * values)))
    )


def contract_rows(left, right):
    return lax.dot_general(
        left, right, (((0,), (0,)), ((), ())), preferred_element_type=jnp.float32
    )


def contract_cols(left, right):
    return lax.dot_general(
        left, right, (((1,), (1,)), ((), ())), preferred_element_type=jnp.float32
    )


def block_scores(query_block, key_rows, offset, length):
    scale = query_block.shape[2] ** (-0.5)
    scores = (
        jnp.einsum("qhd,kd->hqk", query_block, key_rows, preferred_element_type=jnp.float32) * scale
    )
    rows_pos = offset + jnp.arange(query_block.shape[0], dtype=jnp.int32)
    keys_pos = jnp.arange(key_rows.shape[0], dtype=jnp.int32)
    allowed = (keys_pos[None, :] <= rows_pos[:, None]) & (keys_pos[None, :] < length)
    return jnp.where(allowed[None], scores, -1e30)


def attend_forward(queries, key_rows, value_rows, length, block_rows):
    pieces = []
    log_totals = []
    for offset in range(0, queries.shape[0], block_rows):
        query_block = queries[offset : offset + block_rows]
        scores = block_scores(query_block, key_rows, offset, length)
        highest = jnp.max(scores, axis=-1, keepdims=True)
        exponent = jnp.exp(scores - highest)
        normaliser = jnp.sum(exponent, axis=-1, keepdims=True)
        probability = (exponent / normaliser).astype(jnp.bfloat16)
        log_totals.append(highest + jnp.log(normaliser))
        pieces.append(
            jnp.einsum("hqk,kd->qhd", probability, value_rows, preferred_element_type=jnp.float32)
        )
    return (jnp.concatenate(pieces, axis=0), log_totals)


def attend_backward(queries, key_rows, value_rows, length, block_rows, log_totals, grad_heads):
    scale = queries.shape[2] ** (-0.5)
    query_grads = []
    key_grads = jnp.zeros(key_rows.shape, jnp.float32)
    value_grads = jnp.zeros(value_rows.shape, jnp.float32)
    for counter, offset in enumerate(range(0, queries.shape[0], block_rows)):
        query_block = queries[offset : offset + block_rows]
        grad_block = grad_heads[offset : offset + block_rows]
        scores = block_scores(query_block, key_rows, offset, length)
        probability = jnp.exp(scores - log_totals[counter])
        grad_probs = jnp.einsum(
            "qhd,kd->hqk", grad_block, value_rows, preferred_element_type=jnp.float32
        )
        inner = jnp.sum(probability * grad_probs, axis=-1, keepdims=True)
        grad_scores = (probability * (grad_probs - inner)).astype(jnp.bfloat16)
        query_grads.append(
            (
                jnp.einsum("hqk,kd->qhd", grad_scores, key_rows, preferred_element_type=jnp.float32)
                * scale
            ).astype(jnp.bfloat16)
        )
        key_grads = (
            key_grads
            + jnp.einsum(
                "hqk,qhd->kd", grad_scores, query_block, preferred_element_type=jnp.float32
            )
            * scale
        )
        value_grads = value_grads + jnp.einsum(
            "hqk,qhd->kd",
            probability.astype(jnp.bfloat16),
            grad_block,
            preferred_element_type=jnp.float32,
        )
    return (jnp.concatenate(query_grads, axis=0), key_grads, value_grads)


def local(
    size,
    devices,
    tokens,
    lengths,
    norm1_gain,
    norm1_shift,
    query_weight,
    query_bias,
    keyval_weight,
    value_bias,
    proj_weight,
    proj_bias,
    norm2_gain,
    norm2_shift,
    up_weight,
    up_bias,
    down_weight,
    down_bias,
    cotangent,
):
    wide = jnp.float32
    slot_len, width = tokens.shape
    head_dim = keyval_weight.shape[1] // 2
    heads_here = query_weight.shape[1] // head_dim
    block_rows = min(512, slot_len)
    length = lengths[0]

    def row(vector):
        return vector.astype(wide).reshape(1, -1)

    hidden1 = layer_norm(tokens.astype(wide), norm1_gain.astype(wide), norm1_shift.astype(wide)).astype(jnp.bfloat16)
    queries = (
        jnp.dot(hidden1, query_weight, preferred_element_type=wide) + query_bias.astype(wide)
    ).astype(jnp.bfloat16)
    keyval = jnp.dot(hidden1, keyval_weight, preferred_element_type=wide)
    key_rows = keyval[:, :head_dim].astype(jnp.bfloat16)
    value_rows = (keyval[:, head_dim:] + value_bias.astype(wide)).astype(jnp.bfloat16)
    slot_queries = queries.reshape(slot_len, heads_here, head_dim)
    attended, log_totals = attend_forward(slot_queries, key_rows, value_rows, length, block_rows)
    heads_out = attended.reshape(slot_len, heads_here * head_dim).astype(jnp.bfloat16)
    attn_terms = jnp.dot(heads_out, proj_weight, preferred_element_type=wide).astype(jnp.bfloat16)
    hidden2, mid = reduce_middle(size, attn_terms, tokens, row(proj_bias), row(norm2_gain), row(norm2_shift))

    pre_act = jnp.dot(hidden2, up_weight, preferred_element_type=wide) + up_bias.astype(wide)
    activated = gelu_tanh(pre_act).astype(jnp.bfloat16)
    valid = (jnp.arange(slot_len, dtype=jnp.int32) < length)[:, None]
    d_out = jnp.where(valid, cotangent, jnp.zeros_like(cotangent))
    grad_down = contract_rows(activated, d_out).astype(jnp.bfloat16)
    grad_down = lax.psum(grad_down, "dp")
    grad_act = contract_cols(d_out, down_weight).astype(jnp.bfloat16)
    gelu_pull = jax.vjp(gelu_tanh, pre_act)[1]
    grad_pre = gelu_pull(grad_act.astype(wide))[0].astype(jnp.bfloat16)
    back2 = contract_cols(grad_pre, up_weight).astype(jnp.bfloat16)
    middle_low, dmid, sums2 = reduce_back(size, back2, d_out, mid, row(norm2_gain))
    if up_weight.shape[1] == width:
        grad_up = contract_rows(hidden2, grad_pre).astype(jnp.bfloat16)
    else:
        grad_up = contract_rows(grad_pre, hidden2).astype(jnp.bfloat16)
    grad_upbias = jnp.sum(grad_pre.astype(wide), axis=0)
    mlp_terms = jnp.dot(activated, down_weight, preferred_element_type=wide).astype(jnp.bfloat16)

    grad_proj = contract_rows(heads_out, middle_low).astype(jnp.bfloat16)
    grad_heads = contract_cols(middle_low, proj_weight).astype(jnp.bfloat16)
    slot_grads = grad_heads.reshape(slot_len, heads_here, head_dim)
    query_part, key_part, value_part = attend_backward(
        slot_queries, key_rows, value_rows, length, block_rows, log_totals, slot_grads
    )
    grad_queries = query_part.reshape(slot_len, heads_here * head_dim)
    grad_kv_rows = jnp.concatenate([key_part, value_part], axis=1).astype(jnp.bfloat16)
    grad_qbias = jnp.sum(grad_queries.astype(wide), axis=0)
    grad_query = contract_rows(grad_queries, hidden1).astype(jnp.bfloat16)
    grad_keyval = contract_rows(grad_kv_rows, hidden1).astype(jnp.bfloat16)
    grad_vbias = jnp.sum(grad_kv_rows[:, head_dim:].astype(wide), axis=0)
    back1 = (
        contract_cols(grad_queries, query_weight) + contract_cols(grad_kv_rows, keyval_weight)
    ).astype(jnp.bfloat16)

    def padded(vector):
        return jnp.pad(vector, (0, width - vector.shape[0])).reshape(1, width)

    small = jnp.concatenate(
        [
            jnp.zeros((2, width), wide),
            jnp.sum(sums2, axis=1),
            padded(grad_vbias),
            jnp.zeros((1, width), wide),
            padded(grad_qbias),
            padded(grad_upbias),
            jnp.zeros((6, width), wide),
        ]
    )
    arrays = (grad_up, grad_proj, grad_query, grad_keyval)
    result, grad_tokens, total, small = reduce_last(
        size,
        devices,
        mlp_terms,
        back1,
        grad_keyval,
        tokens,
        mid,
        dmid,
        row(down_bias),
        row(norm1_gain),
        small,
        arrays[:3],
    )
    ends = [0]
    for array in arrays:
        ends.append(ends[-1] + array.shape[0])
    grad_up, grad_proj, grad_query, kv_sum = (total[low:high] for low, high in zip(ends, ends[1:]))
    if up_weight.shape[1] != width:
        grad_up = grad_up.T
    grad_gain1, grad_shift1, grad_gain2, grad_shift2, grad_pbias, grad_dnbias = (
        small[place] for place in range(6)
    )
    grad_vbias = small[6, :head_dim]
    grad_qbias = small[8, : query_bias.shape[0]]
    grad_upbias = small[9, : up_bias.shape[0]]
    return (
        result,
        grad_tokens,
        grad_gain1,
        grad_shift1,
        grad_query.T.astype(wide),
        grad_qbias,
        kv_sum.T.astype(wide),
        grad_vbias,
        grad_proj.astype(wide),
        grad_pbias,
        grad_gain2,
        grad_shift2,
        grad_up.astype(wide),
        grad_upbias,
        grad_down.astype(wide),
        grad_dnbias,
    )


def solution(mesh):
    in_specs = (
        P("dp", None),
        P("dp"),
        P(),
        P(),
        P(None, "tensor"),
        P("tensor"),
        P(),
        P(),
        P("tensor", None),
        P(),
        P(),
        P(),
        P(None, "tensor"),
        P("tensor"),
        P("tensor", None),
        P(),
        P("dp", None),
    )
    out_specs = (
        P("dp", None),
        P("dp", None),
        P(),
        P(),
        P(None, "tensor"),
        P("tensor"),
        P(),
        P(),
        P("tensor", None),
        P(),
        P(),
        P(),
        P(None, "tensor"),
        P("tensor"),
        P("tensor", None),
        P(),
    )
    return jax.shard_map(functools.partial(local, mesh.shape["tensor"], mesh.shape["dp"]), mesh=mesh, in_specs=in_specs, out_specs=out_specs, check_vma=False)
```

```python
import functools

import jax
import jax.numpy as jnp
from jax import lax
from jax.experimental import pallas as pl
from jax.experimental.pallas import tpu as pltpu
from jax.sharding import PartitionSpec as P

STRIP = 16
EPS = 1e-05


def suffixes(count):
    if count == 0:
        return [()]
    rest = [()]
    for _ in range(count - 1):
        rest = [(bit,) + more for bit in (1, 0) for more in rest]
    return [(bit,) + more for bit in (1, 0) for more in rest]


def pieces(unit):
    return 2 if unit % (2 * STRIP) == 0 else 1


def as_number(path):
    total = 0
    for bit in path:
        total = 2 * total + bit
    return total


class Tree:
    def __init__(self, axis, size, number, rows):
        self.axis, self.size = axis, size
        self.depth = size.bit_length() - 1
        self.number = number
        self.half = rows // 2
        self.unit = self.half // size
        order = list(range(self.depth))
        self.order = order if number == 0 else order[::-1]
        me = lax.axis_index(axis)
        self.mine = [(me // (1 << bit)) % 2 for bit in self.order]
        self.partners = [me + (1 - 2 * own) * (1 << bit) for own, bit in zip(self.mine, self.order)]

    def offset(self, path, skip=0):
        start = 0
        for level in range(skip, self.depth):
            side = (self.mine[level] + path[level]) % 2
            start = start + side * (self.half >> (level + 1))
        return start

    def rows(self, path, sub, sub_rows):
        start = self.number * self.half + self.offset(path) + sub * sub_rows
        return pl.ds(pl.multiple_of(start, sub_rows), sub_rows)

    def own_rows(self, path, sub, sub_rows):
        start = self.offset(path, 1) + sub * sub_rows
        return pl.multiple_of(start, sub_rows)

    def slot(self, level, path):
        base = sum(1 << (self.depth - 1 - lower) for lower in range(level))
        return base + as_number(path)


def stream(axis, size, shape, part, out, own, slots, outbuf, local_sem, send_sem, recv_sem, finish, loads=()):
    rows, width = shape
    trees = [Tree(axis, size, number, rows) for number in (0, 1)]
    unit = trees[0].unit
    depth = trees[0].depth
    subs = pieces(unit)
    sub_rows = unit // subs
    sends = []

    def remote(tree, src, dst, kind, index, sub, level):
        place = ((tree.number * 2 + kind) * (size - 1) + index) * subs + sub
        copy = pltpu.make_async_remote_copy(
            src_ref=src,
            dst_ref=dst,
            send_sem=send_sem.at[place],
            recv_sem=recv_sem.at[place],
            device_id={axis: tree.partners[level]},
            device_id_type=pl.DeviceIdType.MESH,
        )
        return copy

    def reduce_copy(tree, level, path, sub):
        slot = tree.slot(level, path)
        if level == 0:
            src = part.at[tree.rows((1,) + path, sub, sub_rows), :]
        else:
            src = slots.at[tree.number, tree.slot(level - 1, (1,) + path), pl.ds(sub * sub_rows, sub_rows), :]
        dst = slots.at[tree.number, slot, pl.ds(sub * sub_rows, sub_rows), :]
        return remote(tree, src, dst, 0, slot, sub, level)

    def gather_copy(tree, level, path, sub):
        there = path[:level] + (1,) + path[level + 1 :]
        where = tree.rows(path, sub, sub_rows)
        if any(path):
            src = out.at[where, :]
        else:
            src = outbuf.at[tree.number, pl.ds(sub * sub_rows, sub_rows), :]
        return remote(tree, src, out.at[where, :], 1, as_number(there) - 1, sub, level)

    copies = []
    for tree in trees:
        start = tree.number * tree.half + tree.mine[0] * (tree.half // 2)
        copies.append(
            pltpu.make_async_copy(
                part.at[pl.ds(pl.multiple_of(start, tree.half // 2), tree.half // 2), :],
                own.at[tree.number],
                local_sem.at[tree.number],
            )
        )
    for copy in copies:
        copy.start()
    for path in suffixes(depth - 1):
        for sub in range(subs):
            for tree in trees:
                copy = reduce_copy(tree, 0, path, sub)
                copy.start()
                sends.append(copy)
    for copy in copies:
        copy.wait()
    yield True
    zero = (0,) * depth
    stored = []
    for level in range(depth):
        last = level == depth - 1
        if last:
            for load in loads:
                load.wait()
        paths = suffixes(depth - 1 - level)
        for path in paths:
            for sub in range(subs):
                for tree in trees:
                    reduce_copy(tree, level, path, sub).wait_recv()
                    slot = tree.slot(level, path)
                    first = tree.own_rows((0,) + path if level == 0 else zero, sub, sub_rows)

                    def strip(step, tree=tree, slot=slot, first=first, path=path, sub=sub, level=level, last=last):
                        line = sub * sub_rows + step * STRIP
                        here = pl.ds(pl.multiple_of(line, STRIP), STRIP)
                        if level == 0:
                            mine = own[tree.number, pl.ds(pl.multiple_of(first + step * STRIP, STRIP), STRIP), :]
                        else:
                            mine = slots[tree.number, tree.slot(level - 1, (0,) + path), here, :]
                        total = mine.astype(jnp.float32) + slots[tree.number, slot, here, :].astype(jnp.float32)
                        if last:
                            outbuf[tree.number, here, :] = finish(
                                total, tree.number, here, pl.ds(pl.multiple_of(tree.number * unit + line, STRIP), STRIP)
                            )
                        else:
                            slots[tree.number, slot, here, :] = total.astype(slots.dtype)

                    pl.loop(0, sub_rows // STRIP)(strip)
                    if last:
                        keep = pltpu.make_async_copy(
                            outbuf.at[tree.number, pl.ds(sub * sub_rows, sub_rows), :],
                            out.at[tree.rows(zero, sub, sub_rows), :],
                            local_sem.at[2 + tree.number * subs + sub],
                        )
                        keep.start()
                        stored.append(keep)
                        for back in reversed(range(depth)):
                            copy = gather_copy(tree, back, zero, sub)
                            copy.start()
                            sends.append(copy)
                    elif path[0] == 1:
                        copy = reduce_copy(tree, level + 1, path[1:], sub)
                        copy.start()
                        sends.append(copy)
                yield path == paths[-1] and sub == subs - 1
    for level in reversed(range(depth)):
        paths = suffixes(depth - 1 - level)
        for path in paths:
            full = (0,) * level + (1,) + path
            sender = (0,) * (level + 1) + path
            for sub in range(subs):
                for tree in trees:
                    gather_copy(tree, level, sender, sub).wait_recv()
                    for back in reversed(range(level)):
                        copy = gather_copy(tree, back, full, sub)
                        copy.start()
                        sends.append(copy)
                yield path == paths[-1] and sub == subs - 1
    for copy in sends:
        copy.wait_send()
    for copy in stored:
        copy.wait()


def greet(axis, size):
    barrier = pltpu.get_barrier_semaphore()
    me = lax.axis_index(axis)
    for step in range(1, size):
        pl.semaphore_signal(
            barrier, inc=1, device_id={axis: (me + step) % size}, device_id_type=pl.DeviceIdType.MESH
        )
    pl.semaphore_wait(barrier, size - 1)


def run_together(streams):
    waiting = list(streams)
    while waiting:
        left = []
        for one in waiting:
            try:
                next(one)
                left.append(one)
            except StopIteration:
                pass
        waiting = left


def stream_scratch(size, rows, width):
    half = rows // 2
    unit = half // size
    subs = pieces(unit)
    count = 2 * 2 * (size - 1) * subs
    return [
        pltpu.VMEM((2, half // 2, width), jnp.bfloat16),
        pltpu.VMEM((2, size - 1, unit, width), jnp.bfloat16),
        pltpu.VMEM((2, unit, width), jnp.bfloat16),
        pltpu.SemaphoreType.DMA((2 + 2 * subs,)),
        pltpu.SemaphoreType.DMA((count,)),
        pltpu.SemaphoreType.DMA((count,)),
    ]


def load_rows(axis, size, rows, source, target, sems):
    copies = []
    for number in (0, 1):
        tree = Tree(axis, size, number, rows)
        unit = tree.unit
        copies.append(
            pltpu.make_async_copy(
                source.at[tree.rows((0,) * tree.depth, 0, unit), :], target.at[number], sems.at[number]
            )
        )
    for copy in copies:
        copy.start()
    return copies


def moments(values):
    center = values - jnp.mean(values, axis=-1, keepdims=True)
    scale = lax.rsqrt(jnp.mean(center * center, axis=-1, keepdims=True) + EPS)
    return center * scale, scale


def norm_back(grad, gain, scaled, scale):
    inner = grad * gain
    return scale * (
        inner
        - jnp.mean(inner, axis=-1, keepdims=True)
        - scaled * jnp.mean(inner * scaled, axis=-1, keepdims=True)
    )


def fold(values):
    return values[:8] + values[8:]


BLOCK = 256


def block_of(index):
    return pl.ds(pl.multiple_of(index * BLOCK, BLOCK), BLOCK)


def plain_task(left, right, out, index):
    @pl.loop(0, left.shape[0] // BLOCK)
    def _(step):
        rows = block_of(step)
        out[rows, block_of(index)] = jnp.dot(
            left[rows, :], right[:, block_of(index)], preferred_element_type=jnp.float32
        ).astype(out.dtype)


def flipped_task(left, right, out, index):
    @pl.loop(0, left.shape[0] // BLOCK)
    def _(step):
        rows = block_of(step)
        out[rows, block_of(index)] = contract_cols(left[rows, :], right[block_of(index), :]).astype(out.dtype)


def rows_task(left, right, out, turned, index):
    turned[...] = left[:, block_of(index)].T

    @pl.loop(0, right.shape[1] // BLOCK)
    def _(step):
        columns = block_of(step)
        out[block_of(index), columns] = jnp.dot(
            turned[...], right[:, columns], preferred_element_type=jnp.float32
        ).astype(out.dtype)


def widen(array, start, rows):
    width = array.shape[1]

    def body(source, target):
        target[...] = source[...].astype(jnp.float32)

    return pl.pallas_call(
        body,
        grid=(rows // BLOCK,),
        out_shape=jax.ShapeDtypeStruct((rows, width), jnp.float32),
        in_specs=[pl.BlockSpec((BLOCK, width), lambda step: (step + start // BLOCK, 0))],
        out_specs=pl.BlockSpec((BLOCK, width), lambda step: (step, 0)),
        name="widen",
    )(array)


def products(sources, targets, load_sems, store_sems, jobs, early=()):
    loads = [pltpu.make_async_copy(src, dst, load_sems.at[place]) for place, (src, dst) in enumerate(zip(sources, targets))]
    for load in loads:
        load.start()
    yield
    waited = set()
    stores = []
    for needs, task, out, where, index in jobs:
        for place in needs:
            if place not in waited:
                waited.add(place)
                loads[place].wait()
        task(index)
        held = out[0].at[block_of(index), :] if where == 0 else out[0].at[:, block_of(index)]
        there = out[1].at[block_of(index), :] if where == 0 else out[1].at[:, block_of(index)]
        store = pltpu.make_async_copy(held, there, store_sems.at[len(stores)])
        store.start()
        stores.append(store)
        if len(stores) not in early:
            yield
    for store in stores:
        store.wait()


HBM = pl.BlockSpec(memory_space=pl.ANY)
VMEM = pl.BlockSpec(memory_space=pltpu.VMEM)


def middle_kernel(size, rows, width, part, tokens, pbias, gain, shift, d_out, down, hidden, mid, act, own, slots, outbuf, local_sem, send_sem, recv_sem, tok, load_sem, *work):
    dout_here, down_here, act_here, in_sem, out_sem = work
    greet("tensor", size)
    loads = load_rows("tensor", size, rows, tokens, tok, load_sem)

    def finish(total, number, here, line):
        value = tok[number, here, :].astype(jnp.float32) + total + pbias[...]
        mid[line, :] = value
        scaled, _ = moments(value)
        return (scaled * gain[...] + shift[...]).astype(jnp.bfloat16)

    jobs = [
        ((0, 1), functools.partial(flipped_task, dout_here, down_here, act_here), (act_here, act), 1, index)
        for index in range(down.shape[0] // BLOCK)
    ]
    run_together(
        [
            stream("tensor", size, (rows, width), part, hidden, own, slots, outbuf, local_sem, send_sem, recv_sem, finish, loads),
            products((d_out, down), (dout_here, down_here), in_sem, out_sem, jobs),
        ]
    )


def reduce_middle(size, part, tokens, pbias, gain, shift, d_out, down):
    rows, width = part.shape
    units = down.shape[0]
    unit = rows // 2 // size
    return pl.pallas_call(
        functools.partial(middle_kernel, size, rows, width),
        out_shape=(
            jax.ShapeDtypeStruct((rows, width), jnp.bfloat16),
            jax.ShapeDtypeStruct((2 * unit, width), jnp.float32),
            jax.ShapeDtypeStruct((rows, units), jnp.bfloat16),
        ),
        in_specs=[HBM, HBM, VMEM, VMEM, VMEM, HBM, HBM],
        out_specs=(HBM, VMEM, HBM),
        scratch_shapes=stream_scratch(size, rows, width)
        + [pltpu.VMEM((2, unit, width), jnp.bfloat16), pltpu.SemaphoreType.DMA((2,))]
        + [
            pltpu.VMEM((rows, width), jnp.bfloat16),
            pltpu.VMEM((units, width), jnp.bfloat16),
            pltpu.VMEM((rows, units), jnp.bfloat16),
            pltpu.SemaphoreType.DMA((2,)),
            pltpu.SemaphoreType.DMA((units // BLOCK,)),
        ],
        compiler_params=pltpu.CompilerParams(
            collective_id=1, has_side_effects=True, vmem_limit_bytes=60 * 1024 * 1024
        ),
        name="reduce_middle",
    )(part, tokens, pbias, gain, shift, d_out, down)


def back_kernel(size, rows, width, part, d_out, mid, gain, act, down, hidden, pre, low, dmid, sums, mlp, grad_up, own, slots, outbuf, local_sem, send_sem, recv_sem, dout, load_sem, *work):
    act_here, down_here, hidden_here, pre_here, mlp_here, up_here, turned, in_sem, out_sem = work
    greet("tensor", size)
    loads = load_rows("tensor", size, rows, d_out, dout, load_sem)
    sums[...] = jnp.zeros_like(sums)

    def finish(total, number, here, line):
        scaled, scale = moments(mid[line, :])
        direct = dout[number, here, :].astype(jnp.float32)
        value = direct + norm_back(total, gain[...], scaled, scale)
        dmid[line, :] = value
        sums[0] += fold(total * scaled)
        sums[1] += fold(total)
        sums[2] += fold(value)
        sums[3] += fold(direct)
        return value.astype(jnp.bfloat16)

    jobs = [
        ((0, 1), functools.partial(plain_task, act_here, down_here, mlp_here), (mlp_here, mlp), 1, index)
        for index in range(width // BLOCK)
    ] + [
        ((2, 3), functools.partial(rows_task, hidden_here, pre_here, up_here, turned), (up_here, grad_up), 0, index)
        for index in range(width // BLOCK)
    ]
    run_together(
        [
            stream("tensor", size, (rows, width), part, low, own, slots, outbuf, local_sem, send_sem, recv_sem, finish, loads),
            products(
                (act, down, hidden, pre), (act_here, down_here, hidden_here, pre_here), in_sem, out_sem, jobs, (1, 2, 4, 5, 7, 8)
            ),
        ]
    )


def reduce_back(size, part, d_out, mid, gain, act, down, hidden, pre):
    rows, width = part.shape
    units = down.shape[0]
    unit = rows // 2 // size
    return pl.pallas_call(
        functools.partial(back_kernel, size, rows, width),
        out_shape=(
            jax.ShapeDtypeStruct((rows, width), jnp.bfloat16),
            jax.ShapeDtypeStruct((2 * unit, width), jnp.float32),
            jax.ShapeDtypeStruct((4, 8, width), jnp.float32),
            jax.ShapeDtypeStruct((rows, width), jnp.bfloat16),
            jax.ShapeDtypeStruct((width, units), jnp.bfloat16),
        ),
        in_specs=[HBM, HBM, VMEM, VMEM, HBM, HBM, HBM, HBM],
        out_specs=(HBM, VMEM, VMEM, HBM, HBM),
        scratch_shapes=stream_scratch(size, rows, width)
        + [pltpu.VMEM((2, unit, width), jnp.bfloat16), pltpu.SemaphoreType.DMA((2,))]
        + [
            pltpu.VMEM((rows, units), jnp.bfloat16),
            pltpu.VMEM((units, width), jnp.bfloat16),
            pltpu.VMEM((rows, width), jnp.bfloat16),
            pltpu.VMEM((rows, units), jnp.bfloat16),
            pltpu.VMEM((rows, width), jnp.bfloat16),
            pltpu.VMEM((width, units), jnp.bfloat16),
            pltpu.VMEM((BLOCK, rows), jnp.bfloat16),
            pltpu.SemaphoreType.DMA((4,)),
            pltpu.SemaphoreType.DMA((2 * (width // BLOCK),)),
        ],
        compiler_params=pltpu.CompilerParams(
            collective_id=2, has_side_effects=True, vmem_limit_bytes=60 * 1024 * 1024
        ),
        name="reduce_back",
    )(part, d_out, mid, gain, act, down, hidden, pre)


def remote_copy(axis, target, src, dst, send_sem, recv_sem):
    return pltpu.make_async_remote_copy(
        src_ref=src,
        dst_ref=dst,
        send_sem=send_sem,
        recv_sem=recv_sem,
        device_id={axis: target},
        device_id_type=pl.DeviceIdType.MESH,
    )


CHUNK = 32
SKEW = 1
CORE_SEND, CORE_RECV, UP_SEND, LEFT_RECV, RIGHT_RECV, BACK_LEFT, BACK_RIGHT, BACK_RECV, TWIN_SEND, TWIN_RECV, KEEP, LOAD = range(12)


def chain_scratch(rows, width):
    half = rows // 2
    return [pltpu.VMEM((half, width), jnp.bfloat16)] * 4 + [pltpu.SemaphoreType.DMA((12, half // CHUNK))]


def chain(devices, sources, out, own, twin, left, right, sems):
    length = devices // 2
    me = lax.axis_index("dp")
    core, place = me % 2, me // 2
    other = me + 1 - 2 * core
    deepest = length // 2

    def at(ref, chunk):
        return ref.at[pl.ds(pl.multiple_of(chunk * CHUNK, CHUNK), CHUNK), :]

    def part(ref, side, chunk):
        return ref.at[pl.ds(pl.multiple_of((2 * chunk + side) * CHUNK, CHUNK), CHUNK), :]

    def core_copy(source, chunk, first):
        return remote_copy("dp", other, part(source, 1 - core, chunk - first), at(twin, chunk), sems.at[CORE_SEND, chunk], sems.at[CORE_RECV, chunk])

    def load(source, chunk, first):
        return pltpu.make_async_copy(part(source, core, chunk - first), at(own, chunk), sems.at[LOAD, chunk])

    def to_right(chunk):
        return remote_copy("dp", me + 2, at(own, chunk), at(left, chunk), sems.at[UP_SEND, chunk], sems.at[LEFT_RECV, chunk])

    def to_left(chunk):
        return remote_copy("dp", me - 2, at(own, chunk), at(right, chunk), sems.at[UP_SEND, chunk], sems.at[RIGHT_RECV, chunk])

    def spread(chunk, src, step, send):
        return remote_copy("dp", me + step, src, part(out, core, chunk), sems.at[send, chunk], sems.at[BACK_RECV, chunk])

    def twin_copy(chunk, src):
        return remote_copy("dp", other, src, part(out, core, chunk), sems.at[TWIN_SEND, chunk], sems.at[TWIN_RECV, chunk])

    def twin_arrival(chunk):
        there = part(out, 1 - core, chunk)
        return remote_copy("dp", other, there, there, sems.at[TWIN_SEND, chunk], sems.at[TWIN_RECV, chunk])

    def keep(chunk):
        return pltpu.make_async_copy(at(own, chunk), part(out, core, chunk), sems.at[KEEP, chunk])

    def add(chunk, terms):
        def strip(step):
            line = pl.ds(pl.multiple_of(chunk * CHUNK + step * STRIP, STRIP), STRIP)
            total = own[line, :].astype(jnp.float32)
            for term in terms:
                total = total + term[line, :].astype(jnp.float32)
            own[line, :] = total.astype(own.dtype)

        pl.loop(0, CHUNK // STRIP)(strip)

    def gather_up(chunk, goal):
        core_copy(out, chunk, 0).wait_recv()
        load(out, chunk, 0).wait()
        has_left = (place > 0) & (place <= goal)
        has_right = (place < length - 1) & (place >= goal)

        @pl.when(~has_right & ~has_left)
        def _():
            add(chunk, [twin])

        @pl.when(has_left & ~has_right)
        def _():
            to_right(chunk).wait_recv()
            add(chunk, [twin, left])

        @pl.when(has_right & ~has_left)
        def _():
            to_left(chunk).wait_recv()
            add(chunk, [twin, right])

        @pl.when(has_left & has_right)
        def _():
            to_right(chunk).wait_recv()
            to_left(chunk).wait_recv()
            add(chunk, [twin, left, right])

        @pl.when(place < goal)
        def _():
            to_right(chunk).start()

        @pl.when(place > goal)
        def _():
            to_left(chunk).start()

        @pl.when(place == goal)
        def _():
            @pl.when(place > 0)
            def _():
                spread(chunk, at(own, chunk), -2, BACK_LEFT).start()

            @pl.when(place < length - 1)
            def _():
                spread(chunk, at(own, chunk), 2, BACK_RIGHT).start()

            twin_copy(chunk, at(own, chunk)).start()
            keep(chunk).start()

    def hand_back(chunk, goal):
        here = part(out, core, chunk)

        @pl.when(place < goal)
        def _():
            spread(chunk, here, 2, BACK_RIGHT).wait_recv()

            @pl.when(place > 0)
            def _():
                spread(chunk, here, -2, BACK_LEFT).start()

            twin_copy(chunk, here).start()

        @pl.when(place > goal)
        def _():
            spread(chunk, here, -2, BACK_LEFT).wait_recv()

            @pl.when(place < length - 1)
            def _():
                spread(chunk, here, 2, BACK_RIGHT).start()

            twin_copy(chunk, here).start()

    def finish(chunk, goal):
        here = part(out, core, chunk)
        core_copy(out, chunk, 0).wait_send()
        twin_arrival(chunk).wait_recv()
        twin_copy(chunk, here).wait_send()

        @pl.when(place < goal)
        def _():
            to_right(chunk).wait_send()

        @pl.when(place > goal)
        def _():
            to_left(chunk).wait_send()

        @pl.when((place <= goal) & (place > 0))
        def _():
            spread(chunk, here, -2, BACK_LEFT).wait_send()

        @pl.when((place >= goal) & (place < length - 1))
        def _():
            spread(chunk, here, 2, BACK_RIGHT).wait_send()

        @pl.when(place == goal)
        def _():
            keep(chunk).wait()

    def open_source(source, first, count):
        @pl.loop(first, first + count)
        def _(chunk):
            core_copy(source, chunk, first).start()
            load(source, chunk, first).start()

    late = []
    first = 0
    for source, rows, before in sources:
        count = rows // 2 // CHUNK
        if before is None:
            open_source(source, first, count)
        else:
            late.append((source, first, count, before))
        first += count
    pairs = first // 2
    yield
    for step in range(pairs + SKEW * 2 * deepest):
        for source, begin, count, before in late:
            if step == max(0, begin // 2 - 2):
                for _ in before:
                    pass
                open_source(source, begin, count)
        for parity in (0, 1):
            goal = deepest - 1 + parity
            below = (place < goal).astype(jnp.int32)
            above = (place > goal).astype(jnp.int32)
            level = below * place + above * (length - 1 - place) + (1 - below - above) * deepest
            pair = step - SKEW * level

            @pl.when((pair >= 0) & (pair < pairs))
            def _(parity=parity, goal=goal, pair=pair):
                gather_up(2 * pair + parity, goal)

            away = below * (goal - place) + above * (place - goal)
            pair_back = step - SKEW * (deepest + away)

            @pl.when((away > 0) & (pair_back >= 0) & (pair_back < pairs))
            def _(parity=parity, goal=goal, pair_back=pair_back):
                hand_back(2 * pair_back + parity, goal)

        yield

    @pl.loop(0, pairs)
    def _(pair):
        finish(2 * pair, deepest - 1)
        finish(2 * pair + 1, deepest)


def small_scratch(size, devices, width):
    return [
        pltpu.VMEM((size, 8, width), jnp.float32),
        pltpu.VMEM((devices, 16, width), jnp.float32),
        pltpu.SemaphoreType.DMA((2, size)),
        pltpu.SemaphoreType.DMA((2, devices)),
    ]


def small_sum(size, devices, turns, given, sums, out, near, far, near_sem, far_sem):
    def send(axis, members, slots, sem):
        me = lax.axis_index(axis)
        copies = []
        for step in range(1, members):
            target = (me + step) % members
            copy = remote_copy(axis, target, slots.at[me], slots.at[me], sem.at[0, target], sem.at[1, me])
            copy.start()
            copies.append(copy)
        return copies

    def receive(axis, members, slots, sem, copies):
        me = lax.axis_index(axis)
        for step in range(1, members):
            source = (me + step) % members
            remote_copy(axis, source, slots.at[source], slots.at[source], sem.at[0, source], sem.at[1, source]).wait_recv()
        for copy in copies:
            copy.wait_send()

    for _ in range(turns):
        yield True
    mine = given[0:8, :]
    row = lax.broadcasted_iota(jnp.int32, mine.shape, 0)
    mine = jnp.where(row == 0, jnp.sum(sums[0], axis=0, keepdims=True), mine)
    mine = jnp.where(row == 1, jnp.sum(sums[1], axis=0, keepdims=True), mine)
    near[lax.axis_index("tensor")] = mine
    copies = send("tensor", size, near, near_sem)
    yield True
    receive("tensor", size, near, near_sem, copies)
    total = near[0]
    for member in range(1, size):
        total = total + near[member]
    me = lax.axis_index("dp")
    far[me, 0:8, :] = total
    far[me, 8:16, :] = given[8:16, :]
    copies = send("dp", devices, far, far_sem)
    yield False
    yield False
    receive("dp", devices, far, far_sem, copies)
    total = far[0]
    for member in range(1, devices):
        total = total + far[member]
    out[...] = total


def in_turns(*parts):
    waiting = list(parts)
    while waiting:
        left = []
        for one, quiet in waiting:
            ended = False
            try:
                while not ended:
                    ended = next(one)
                    if not quiet:
                        yield
                left.append((one, quiet))
            except StopIteration:
                pass
        waiting = left


def greet_all(sizes):
    barrier = pltpu.get_barrier_semaphore()
    total = 0
    for axis, size in sizes:
        me = lax.axis_index(axis)
        for step in range(1, size):
            pl.semaphore_signal(
                barrier, inc=1, device_id={axis: (me + step) % size}, device_id_type=pl.DeviceIdType.MESH
            )
        total += size - 1
    pl.semaphore_wait(barrier, total)


def last_kernel(size, devices, shapes, mlp, part, kv, tokens, mid, dmid, dbias, gain, small, *rest):
    wide, kv_shape, summed = shapes[0], shapes[1], shapes[2:]
    arrays, rest = rest[: len(summed)], rest[len(summed) :]
    result, grad, total, small_out, kv_out, rest = *rest[:5], rest[5:]
    first, second, third, rest = rest[:6], rest[6:12], rest[12:18], rest[18:]
    tok, load_sem, sums, rest = *rest[:3], rest[3:]
    greet_all((("tensor", size), ("dp", devices)))
    loads = load_rows("tensor", size, wide[0], tokens, tok, load_sem)
    sums[...] = jnp.zeros_like(sums)

    def finish_result(total, number, here, line):
        return (mid[line, :] + total + dbias[...]).astype(jnp.bfloat16)

    def finish_grad(total, number, here, line):
        scaled, scale = moments(tok[number, here, :].astype(jnp.float32))
        sums[0] += fold(total * scaled)
        sums[1] += fold(total)
        return (dmid[line, :] + norm_back(total, gain[...], scaled, scale)).astype(jnp.bfloat16)

    def finish_kv(total, number, here, line):
        return total.astype(jnp.bfloat16)

    kv_stream = stream("tensor", size, kv_shape, kv, kv_out, *third, finish_kv)
    sources = [(array, shape[0], None) for array, shape in zip(arrays, summed)]
    sources.append((kv_out, kv_shape[0], kv_stream))
    run_together(
        [
            in_turns(
                (kv_stream, True),
                (stream("tensor", size, wide, part, grad, *second, finish_grad, loads), False),
                (stream("tensor", size, wide, mlp, result, *first, finish_result), False),
                (small_sum(size, devices, size.bit_length() - 1, small, sums, small_out, *rest[:4]), False),
            ),
            chain(devices, sources, total, *rest[4:]),
        ]
    )


def reduce_last(size, devices, mlp, part, kv, tokens, mid, dmid, dbias, gain, small, arrays):
    rows, width = part.shape
    unit = rows // 2 // size
    shapes = (part.shape, kv.shape) + tuple(array.shape for array in arrays)
    lines = sum(shape[0] for shape in shapes[1:])
    low = jnp.bfloat16
    return pl.pallas_call(
        functools.partial(last_kernel, size, devices, shapes),
        out_shape=(
            jax.ShapeDtypeStruct((rows, width), low),
            jax.ShapeDtypeStruct((rows, width), low),
            jax.ShapeDtypeStruct((lines, width), low),
            jax.ShapeDtypeStruct(small.shape, jnp.float32),
            jax.ShapeDtypeStruct(kv.shape, low),
        ),
        in_specs=[HBM] * 4 + [VMEM] * 5 + [HBM] * len(arrays),
        out_specs=(HBM, HBM, HBM, VMEM, HBM),
        scratch_shapes=stream_scratch(size, rows, width) * 2
        + stream_scratch(size, kv.shape[0], width)
        + [
            pltpu.VMEM((2, unit, width), low),
            pltpu.SemaphoreType.DMA((2,)),
            pltpu.VMEM((2, 8, width), jnp.float32),
        ]
        + small_scratch(size, devices, width)
        + chain_scratch(lines, width),
        compiler_params=pltpu.CompilerParams(
            collective_id=3, has_side_effects=True, vmem_limit_bytes=60 * 1024 * 1024
        ),
        name="reduce_last",
    )(mlp, part, kv, tokens, mid, dmid, dbias, gain, small, *arrays)[:4]


def layer_norm(values, gain, shift):
    center = values - jnp.mean(values, axis=-1, keepdims=True)
    scaled = center * lax.rsqrt(jnp.mean(center * center, axis=-1, keepdims=True) + 1e-05)
    return scaled * gain + shift


def gelu_tanh(values):
    return (
        0.5
        * values
        * (1.0 + jnp.tanh(0.7978845608028654 * (values + 0.044715 * values * values * values)))
    )


def contract_rows(left, right):
    return lax.dot_general(
        left, right, (((0,), (0,)), ((), ())), preferred_element_type=jnp.float32
    )


def contract_cols(left, right):
    return lax.dot_general(
        left, right, (((1,), (1,)), ((), ())), preferred_element_type=jnp.float32
    )


def block_scores(query_block, key_rows, offset, length):
    scale = query_block.shape[2] ** (-0.5)
    scores = (
        jnp.einsum("qhd,kd->hqk", query_block, key_rows, preferred_element_type=jnp.float32) * scale
    )
    rows_pos = offset + jnp.arange(query_block.shape[0], dtype=jnp.int32)
    keys_pos = jnp.arange(key_rows.shape[0], dtype=jnp.int32)
    allowed = (keys_pos[None, :] <= rows_pos[:, None]) & (keys_pos[None, :] < length)
    return jnp.where(allowed[None], scores, -1e30)


def attend_forward(queries, key_rows, value_rows, length, block_rows):
    pieces = []
    log_totals = []
    for offset in range(0, queries.shape[0], block_rows):
        query_block = queries[offset : offset + block_rows]
        scores = block_scores(query_block, key_rows, offset, length)
        highest = jnp.max(scores, axis=-1, keepdims=True)
        exponent = jnp.exp(scores - highest)
        normaliser = jnp.sum(exponent, axis=-1, keepdims=True)
        probability = (exponent / normaliser).astype(jnp.bfloat16)
        log_totals.append(highest + jnp.log(normaliser))
        pieces.append(
            jnp.einsum("hqk,kd->qhd", probability, value_rows, preferred_element_type=jnp.float32)
        )
    return (jnp.concatenate(pieces, axis=0), log_totals)


def attend_backward(queries, key_rows, value_rows, length, block_rows, log_totals, grad_heads):
    scale = queries.shape[2] ** (-0.5)
    query_grads = []
    key_grads = jnp.zeros(key_rows.shape, jnp.float32)
    value_grads = jnp.zeros(value_rows.shape, jnp.float32)
    for counter, offset in enumerate(range(0, queries.shape[0], block_rows)):
        query_block = queries[offset : offset + block_rows]
        grad_block = grad_heads[offset : offset + block_rows]
        scores = block_scores(query_block, key_rows, offset, length)
        probability = jnp.exp(scores - log_totals[counter])
        grad_probs = jnp.einsum(
            "qhd,kd->hqk", grad_block, value_rows, preferred_element_type=jnp.float32
        )
        inner = jnp.sum(probability * grad_probs, axis=-1, keepdims=True)
        grad_scores = (probability * (grad_probs - inner)).astype(jnp.bfloat16)
        query_grads.append(
            (
                jnp.einsum("hqk,kd->qhd", grad_scores, key_rows, preferred_element_type=jnp.float32)
                * scale
            ).astype(jnp.bfloat16)
        )
        key_grads = (
            key_grads
            + jnp.einsum(
                "hqk,qhd->kd", grad_scores, query_block, preferred_element_type=jnp.float32
            )
            * scale
        )
        value_grads = value_grads + jnp.einsum(
            "hqk,qhd->kd",
            probability.astype(jnp.bfloat16),
            grad_block,
            preferred_element_type=jnp.float32,
        )
    return (jnp.concatenate(query_grads, axis=0), key_grads, value_grads)


def local(
    size,
    devices,
    tokens,
    lengths,
    norm1_gain,
    norm1_shift,
    query_weight,
    query_bias,
    keyval_weight,
    value_bias,
    proj_weight,
    proj_bias,
    norm2_gain,
    norm2_shift,
    up_weight,
    up_bias,
    down_weight,
    down_bias,
    cotangent,
):
    wide = jnp.float32
    slot_len, width = tokens.shape
    head_dim = keyval_weight.shape[1] // 2
    heads_here = query_weight.shape[1] // head_dim
    block_rows = min(512, slot_len)
    length = lengths[0]

    def row(vector):
        return vector.astype(wide).reshape(1, -1)

    hidden1 = layer_norm(tokens.astype(wide), norm1_gain.astype(wide), norm1_shift.astype(wide)).astype(jnp.bfloat16)
    queries = (
        jnp.dot(hidden1, query_weight, preferred_element_type=wide) + query_bias.astype(wide)
    ).astype(jnp.bfloat16)
    keyval = jnp.dot(hidden1, keyval_weight, preferred_element_type=wide)
    key_rows = keyval[:, :head_dim].astype(jnp.bfloat16)
    value_rows = (keyval[:, head_dim:] + value_bias.astype(wide)).astype(jnp.bfloat16)
    slot_queries = queries.reshape(slot_len, heads_here, head_dim)
    attended, log_totals = attend_forward(slot_queries, key_rows, value_rows, length, block_rows)
    heads_out = attended.reshape(slot_len, heads_here * head_dim).astype(jnp.bfloat16)
    attn_terms = jnp.dot(heads_out, proj_weight, preferred_element_type=wide).astype(jnp.bfloat16)
    valid = (jnp.arange(slot_len, dtype=jnp.int32) < length)[:, None]
    d_out = jnp.where(valid, cotangent, jnp.zeros_like(cotangent))
    hidden2, mid, grad_act = reduce_middle(
        size, attn_terms, tokens, row(proj_bias), row(norm2_gain), row(norm2_shift), d_out, down_weight
    )

    pre_act = jnp.dot(hidden2, up_weight, preferred_element_type=wide) + up_bias.astype(wide)
    activated = gelu_tanh(pre_act).astype(jnp.bfloat16)
    grad_down = contract_rows(activated, d_out).astype(jnp.bfloat16)
    grad_down = lax.psum(grad_down, "dp")
    gelu_pull = jax.vjp(gelu_tanh, pre_act)[1]
    grad_pre = gelu_pull(grad_act.astype(wide))[0].astype(jnp.bfloat16)
    back2 = contract_cols(grad_pre, up_weight).astype(jnp.bfloat16)
    middle_low, dmid, sums2, mlp_terms, grad_up = reduce_back(
        size, back2, d_out, mid, row(norm2_gain), activated, down_weight, hidden2, grad_pre
    )
    if up_weight.shape[1] != width:
        grad_up = grad_up.T
    grad_upbias = jnp.sum(grad_pre.astype(wide), axis=0)

    grad_proj = contract_rows(heads_out, middle_low).astype(jnp.bfloat16)
    grad_heads = contract_cols(middle_low, proj_weight).astype(jnp.bfloat16)
    slot_grads = grad_heads.reshape(slot_len, heads_here, head_dim)
    query_part, key_part, value_part = attend_backward(
        slot_queries, key_rows, value_rows, length, block_rows, log_totals, slot_grads
    )
    grad_queries = query_part.reshape(slot_len, heads_here * head_dim)
    grad_kv_rows = jnp.concatenate([key_part, value_part], axis=1).astype(jnp.bfloat16)
    grad_qbias = jnp.sum(grad_queries.astype(wide), axis=0)
    grad_query = contract_rows(grad_queries, hidden1).astype(jnp.bfloat16)
    grad_keyval = contract_rows(grad_kv_rows, hidden1).astype(jnp.bfloat16)
    grad_vbias = jnp.sum(grad_kv_rows[:, head_dim:].astype(wide), axis=0)
    back1 = (
        contract_cols(grad_queries, query_weight) + contract_cols(grad_kv_rows, keyval_weight)
    ).astype(jnp.bfloat16)

    def padded(vector):
        return jnp.pad(vector, (0, width - vector.shape[0])).reshape(1, width)

    small = jnp.concatenate(
        [
            jnp.zeros((2, width), wide),
            jnp.sum(sums2, axis=1),
            padded(grad_vbias),
            jnp.zeros((1, width), wide),
            padded(grad_qbias),
            padded(grad_upbias),
            jnp.zeros((6, width), wide),
        ]
    )
    arrays = (grad_up, grad_proj, grad_query, grad_keyval)
    result, grad_tokens, total, small = reduce_last(
        size,
        devices,
        mlp_terms,
        back1,
        grad_keyval,
        tokens,
        mid,
        dmid,
        row(down_bias),
        row(norm1_gain),
        small,
        arrays[:3],
    )
    ends = [0]
    for array in arrays:
        ends.append(ends[-1] + array.shape[0])
    grad_up, grad_proj, grad_query, kv_sum = (total[low:high] for low, high in zip(ends, ends[1:]))
    grad_up = widen(total, 0, ends[1])
    if up_weight.shape[1] != width:
        grad_up = grad_up.T
    grad_gain1, grad_shift1, grad_gain2, grad_shift2, grad_pbias, grad_dnbias = (
        small[place] for place in range(6)
    )
    grad_vbias = small[6, :head_dim]
    grad_qbias = small[8, : query_bias.shape[0]]
    grad_upbias = small[9, : up_bias.shape[0]]
    return (
        result,
        grad_tokens,
        grad_gain1,
        grad_shift1,
        grad_query.T.astype(wide),
        grad_qbias,
        kv_sum.T.astype(wide),
        grad_vbias,
        grad_proj.astype(wide),
        grad_pbias,
        grad_gain2,
        grad_shift2,
        grad_up,
        grad_upbias,
        widen(grad_down, 0, grad_down.shape[0]),
        grad_dnbias,
    )


def solution(mesh):
    in_specs = (
        P("dp", None),
        P("dp"),
        P(),
        P(),
        P(None, "tensor"),
        P("tensor"),
        P(),
        P(),
        P("tensor", None),
        P(),
        P(),
        P(),
        P(None, "tensor"),
        P("tensor"),
        P("tensor", None),
        P(),
        P("dp", None),
    )
    out_specs = (
        P("dp", None),
        P("dp", None),
        P(),
        P(),
        P(None, "tensor"),
        P("tensor"),
        P(),
        P(),
        P("tensor", None),
        P(),
        P(),
        P(),
        P(None, "tensor"),
        P("tensor"),
        P("tensor", None),
        P(),
    )
    return jax.shard_map(functools.partial(local, mesh.shape["tensor"], mesh.shape["dp"]), mesh=mesh, in_specs=in_specs, out_specs=out_specs, check_vma=False)
```

```python
import functools

import jax
import jax.numpy as jnp
from jax import lax
from jax.experimental import pallas as pl
from jax.experimental.pallas import tpu as pltpu
from jax.sharding import PartitionSpec as P

STRIP = 16
EPS = 1e-05


def suffixes(count):
    if count == 0:
        return [()]
    rest = [()]
    for _ in range(count - 1):
        rest = [(bit,) + more for bit in (1, 0) for more in rest]
    return [(bit,) + more for bit in (1, 0) for more in rest]


def pieces(unit):
    return 2 if unit % (2 * STRIP) == 0 else 1


def as_number(path):
    total = 0
    for bit in path:
        total = 2 * total + bit
    return total


class Tree:
    def __init__(self, axis, size, number, rows):
        self.axis, self.size = axis, size
        self.depth = size.bit_length() - 1
        self.number = number
        self.half = rows // 2
        self.unit = self.half // size
        order = list(range(self.depth))
        self.order = order if number == 0 else order[::-1]
        me = lax.axis_index(axis)
        self.mine = [(me // (1 << bit)) % 2 for bit in self.order]
        self.partners = [me + (1 - 2 * own) * (1 << bit) for own, bit in zip(self.mine, self.order)]

    def offset(self, path, skip=0):
        start = 0
        for level in range(skip, self.depth):
            side = (self.mine[level] + path[level]) % 2
            start = start + side * (self.half >> (level + 1))
        return start

    def rows(self, path, sub, sub_rows):
        start = self.number * self.half + self.offset(path) + sub * sub_rows
        return pl.ds(pl.multiple_of(start, sub_rows), sub_rows)

    def own_rows(self, path, sub, sub_rows):
        start = self.offset(path, 1) + sub * sub_rows
        return pl.multiple_of(start, sub_rows)

    def slot(self, level, path):
        base = sum(1 << (self.depth - 1 - lower) for lower in range(level))
        return base + as_number(path)


def stream(axis, size, shape, part, out, own, slots, outbuf, local_sem, send_sem, recv_sem, finish, loads=()):
    rows, width = shape
    trees = [Tree(axis, size, number, rows) for number in (0, 1)]
    unit = trees[0].unit
    depth = trees[0].depth
    subs = pieces(unit)
    sub_rows = unit // subs
    sends = []

    def remote(tree, src, dst, kind, index, sub, level):
        place = ((tree.number * 2 + kind) * (size - 1) + index) * subs + sub
        copy = pltpu.make_async_remote_copy(
            src_ref=src,
            dst_ref=dst,
            send_sem=send_sem.at[place],
            recv_sem=recv_sem.at[place],
            device_id={axis: tree.partners[level]},
            device_id_type=pl.DeviceIdType.MESH,
        )
        return copy

    def reduce_copy(tree, level, path, sub):
        slot = tree.slot(level, path)
        if level == 0:
            src = part.at[tree.rows((1,) + path, sub, sub_rows), :]
        else:
            src = slots.at[tree.number, tree.slot(level - 1, (1,) + path), pl.ds(sub * sub_rows, sub_rows), :]
        dst = slots.at[tree.number, slot, pl.ds(sub * sub_rows, sub_rows), :]
        return remote(tree, src, dst, 0, slot, sub, level)

    def gather_copy(tree, level, path, sub):
        there = path[:level] + (1,) + path[level + 1 :]
        where = tree.rows(path, sub, sub_rows)
        if any(path):
            src = out.at[where, :]
        else:
            src = outbuf.at[tree.number, pl.ds(sub * sub_rows, sub_rows), :]
        return remote(tree, src, out.at[where, :], 1, as_number(there) - 1, sub, level)

    copies = []
    for tree in trees:
        start = tree.number * tree.half + tree.mine[0] * (tree.half // 2)
        copies.append(
            pltpu.make_async_copy(
                part.at[pl.ds(pl.multiple_of(start, tree.half // 2), tree.half // 2), :],
                own.at[tree.number],
                local_sem.at[tree.number],
            )
        )
    for copy in copies:
        copy.start()
    for path in suffixes(depth - 1):
        for sub in range(subs):
            for tree in trees:
                copy = reduce_copy(tree, 0, path, sub)
                copy.start()
                sends.append(copy)
    for copy in copies:
        copy.wait()
    yield True
    zero = (0,) * depth
    stored = []
    for level in range(depth):
        last = level == depth - 1
        if last:
            for load in loads:
                load.wait()
        paths = suffixes(depth - 1 - level)
        for path in paths:
            for sub in range(subs):
                for tree in trees:
                    reduce_copy(tree, level, path, sub).wait_recv()
                    slot = tree.slot(level, path)
                    first = tree.own_rows((0,) + path if level == 0 else zero, sub, sub_rows)

                    def strip(step, tree=tree, slot=slot, first=first, path=path, sub=sub, level=level, last=last):
                        line = sub * sub_rows + step * STRIP
                        here = pl.ds(pl.multiple_of(line, STRIP), STRIP)
                        if level == 0:
                            mine = own[tree.number, pl.ds(pl.multiple_of(first + step * STRIP, STRIP), STRIP), :]
                        else:
                            mine = slots[tree.number, tree.slot(level - 1, (0,) + path), here, :]
                        total = mine.astype(jnp.float32) + slots[tree.number, slot, here, :].astype(jnp.float32)
                        if last:
                            outbuf[tree.number, here, :] = finish(
                                total, tree.number, here, pl.ds(pl.multiple_of(tree.number * unit + line, STRIP), STRIP)
                            )
                        else:
                            slots[tree.number, slot, here, :] = total.astype(slots.dtype)

                    pl.loop(0, sub_rows // STRIP)(strip)
                    if last:
                        keep = pltpu.make_async_copy(
                            outbuf.at[tree.number, pl.ds(sub * sub_rows, sub_rows), :],
                            out.at[tree.rows(zero, sub, sub_rows), :],
                            local_sem.at[2 + tree.number * subs + sub],
                        )
                        keep.start()
                        stored.append(keep)
                        for back in reversed(range(depth)):
                            copy = gather_copy(tree, back, zero, sub)
                            copy.start()
                            sends.append(copy)
                    elif path[0] == 1:
                        copy = reduce_copy(tree, level + 1, path[1:], sub)
                        copy.start()
                        sends.append(copy)
                yield path == paths[-1] and sub == subs - 1
    order = [(level, path) for level in reversed(range(depth)) for path in suffixes(depth - 1 - level)]
    direct = [(level, path) for level, path in order if not any(path)]
    passed = [(level, path) for level, path in order if any(path)]
    for group in (direct, passed):
        for level, path in group:
            full = (0,) * level + (1,) + path
            sender = (0,) * (level + 1) + path
            for sub in range(subs):
                for tree in trees:
                    gather_copy(tree, level, sender, sub).wait_recv()
                    for back in reversed(range(level)):
                        copy = gather_copy(tree, back, full, sub)
                        copy.start()
                        sends.append(copy)
                yield (level, path) == group[-1] and sub == subs - 1
    for copy in sends:
        copy.wait_send()
    for copy in stored:
        copy.wait()


def greet(axis, size):
    barrier = pltpu.get_barrier_semaphore()
    me = lax.axis_index(axis)
    for step in range(1, size):
        pl.semaphore_signal(
            barrier, inc=1, device_id={axis: (me + step) % size}, device_id_type=pl.DeviceIdType.MESH
        )
    pl.semaphore_wait(barrier, size - 1)


def run_together(streams):
    waiting = list(streams)
    while waiting:
        left = []
        for one in waiting:
            try:
                next(one)
                left.append(one)
            except StopIteration:
                pass
        waiting = left


def stream_scratch(size, rows, width):
    half = rows // 2
    unit = half // size
    subs = pieces(unit)
    count = 2 * 2 * (size - 1) * subs
    return [
        pltpu.VMEM((2, half // 2, width), jnp.bfloat16),
        pltpu.VMEM((2, size - 1, unit, width), jnp.bfloat16),
        pltpu.VMEM((2, unit, width), jnp.bfloat16),
        pltpu.SemaphoreType.DMA((2 + 2 * subs,)),
        pltpu.SemaphoreType.DMA((count,)),
        pltpu.SemaphoreType.DMA((count,)),
    ]


def load_rows(axis, size, rows, source, target, sems):
    copies = []
    for number in (0, 1):
        tree = Tree(axis, size, number, rows)
        unit = tree.unit
        copies.append(
            pltpu.make_async_copy(
                source.at[tree.rows((0,) * tree.depth, 0, unit), :], target.at[number], sems.at[number]
            )
        )
    for copy in copies:
        copy.start()
    return copies


def moments(values):
    center = values - jnp.mean(values, axis=-1, keepdims=True)
    scale = lax.rsqrt(jnp.mean(center * center, axis=-1, keepdims=True) + EPS)
    return center * scale, scale


def norm_back(grad, gain, scaled, scale):
    inner = grad * gain
    return scale * (
        inner
        - jnp.mean(inner, axis=-1, keepdims=True)
        - scaled * jnp.mean(inner * scaled, axis=-1, keepdims=True)
    )


def fold(values):
    return values[:8] + values[8:]


BLOCK = 256


def block_of(index):
    return pl.ds(pl.multiple_of(index * BLOCK, BLOCK), BLOCK)


def plain_task(left, right, out, index):
    @pl.loop(0, left.shape[0] // BLOCK)
    def _(step):
        rows = block_of(step)
        out[rows, block_of(index)] = jnp.dot(
            left[rows, :], right[:, block_of(index)], preferred_element_type=jnp.float32
        ).astype(out.dtype)


def flipped_task(left, right, out, index):
    @pl.loop(0, left.shape[0] // BLOCK)
    def _(step):
        rows = block_of(step)
        out[rows, block_of(index)] = contract_cols(left[rows, :], right[block_of(index), :]).astype(out.dtype)


def rows_task(left, right, out, turned, index):
    turned[...] = left[:, block_of(index)].T

    @pl.loop(0, right.shape[1] // BLOCK)
    def _(step):
        columns = block_of(step)
        out[block_of(index), columns] = jnp.dot(
            turned[...], right[:, columns], preferred_element_type=jnp.float32
        ).astype(out.dtype)


def widen(array, start, rows):
    width = array.shape[1]

    def body(source, target):
        target[...] = source[...].astype(jnp.float32)

    return pl.pallas_call(
        body,
        grid=(rows // BLOCK,),
        out_shape=jax.ShapeDtypeStruct((rows, width), jnp.float32),
        in_specs=[pl.BlockSpec((BLOCK, width), lambda step: (step + start // BLOCK, 0))],
        out_specs=pl.BlockSpec((BLOCK, width), lambda step: (step, 0)),
        name="widen",
    )(array)


def products(sources, targets, load_sems, store_sems, jobs, early=()):
    loads = [pltpu.make_async_copy(src, dst, load_sems.at[place]) for place, (src, dst) in enumerate(zip(sources, targets))]
    for load in loads:
        load.start()
    yield
    waited = set()
    stores = []
    for needs, task, out, where, index in jobs:
        for place in needs:
            if place not in waited:
                waited.add(place)
                loads[place].wait()
        task(index)
        held = out[0].at[block_of(index), :] if where == 0 else out[0].at[:, block_of(index)]
        there = out[1].at[block_of(index), :] if where == 0 else out[1].at[:, block_of(index)]
        store = pltpu.make_async_copy(held, there, store_sems.at[len(stores)])
        store.start()
        stores.append(store)
        if len(stores) not in early:
            yield
    for store in stores:
        store.wait()


HBM = pl.BlockSpec(memory_space=pl.ANY)
VMEM = pl.BlockSpec(memory_space=pltpu.VMEM)


def middle_kernel(size, rows, width, part, tokens, pbias, gain, shift, d_out, down, hidden, mid, act, own, slots, outbuf, local_sem, send_sem, recv_sem, tok, load_sem, *work):
    dout_here, down_here, act_here, in_sem, out_sem = work
    greet("tensor", size)
    loads = load_rows("tensor", size, rows, tokens, tok, load_sem)

    def finish(total, number, here, line):
        value = tok[number, here, :].astype(jnp.float32) + total + pbias[...]
        mid[line, :] = value
        scaled, _ = moments(value)
        return (scaled * gain[...] + shift[...]).astype(jnp.bfloat16)

    jobs = [
        ((0, 1), functools.partial(flipped_task, dout_here, down_here, act_here), (act_here, act), 1, index)
        for index in range(down.shape[0] // BLOCK)
    ]
    run_together(
        [
            stream("tensor", size, (rows, width), part, hidden, own, slots, outbuf, local_sem, send_sem, recv_sem, finish, loads),
            products((d_out, down), (dout_here, down_here), in_sem, out_sem, jobs),
        ]
    )


def reduce_middle(size, part, tokens, pbias, gain, shift, d_out, down):
    rows, width = part.shape
    units = down.shape[0]
    unit = rows // 2 // size
    return pl.pallas_call(
        functools.partial(middle_kernel, size, rows, width),
        out_shape=(
            jax.ShapeDtypeStruct((rows, width), jnp.bfloat16),
            jax.ShapeDtypeStruct((2 * unit, width), jnp.float32),
            jax.ShapeDtypeStruct((rows, units), jnp.bfloat16),
        ),
        in_specs=[HBM, HBM, VMEM, VMEM, VMEM, HBM, HBM],
        out_specs=(HBM, VMEM, HBM),
        scratch_shapes=stream_scratch(size, rows, width)
        + [pltpu.VMEM((2, unit, width), jnp.bfloat16), pltpu.SemaphoreType.DMA((2,))]
        + [
            pltpu.VMEM((rows, width), jnp.bfloat16),
            pltpu.VMEM((units, width), jnp.bfloat16),
            pltpu.VMEM((rows, units), jnp.bfloat16),
            pltpu.SemaphoreType.DMA((2,)),
            pltpu.SemaphoreType.DMA((units // BLOCK,)),
        ],
        compiler_params=pltpu.CompilerParams(
            collective_id=1, has_side_effects=True, vmem_limit_bytes=60 * 1024 * 1024
        ),
        name="reduce_middle",
    )(part, tokens, pbias, gain, shift, d_out, down)


def back_kernel(size, rows, width, part, d_out, mid, gain, act, down, hidden, pre, low, dmid, sums, mlp, grad_up, own, slots, outbuf, local_sem, send_sem, recv_sem, dout, load_sem, *work):
    act_here, down_here, hidden_here, pre_here, mlp_here, up_here, turned, in_sem, out_sem = work
    greet("tensor", size)
    loads = load_rows("tensor", size, rows, d_out, dout, load_sem)
    sums[...] = jnp.zeros_like(sums)

    def finish(total, number, here, line):
        scaled, scale = moments(mid[line, :])
        direct = dout[number, here, :].astype(jnp.float32)
        value = direct + norm_back(total, gain[...], scaled, scale)
        dmid[line, :] = value
        sums[0] += fold(total * scaled)
        sums[1] += fold(total)
        sums[2] += fold(value)
        sums[3] += fold(direct)
        return value.astype(jnp.bfloat16)

    jobs = [
        ((0, 1), functools.partial(plain_task, act_here, down_here, mlp_here), (mlp_here, mlp), 1, index)
        for index in range(width // BLOCK)
    ] + [
        ((2, 3), functools.partial(rows_task, hidden_here, pre_here, up_here, turned), (up_here, grad_up), 0, index)
        for index in range(width // BLOCK)
    ]
    run_together(
        [
            stream("tensor", size, (rows, width), part, low, own, slots, outbuf, local_sem, send_sem, recv_sem, finish, loads),
            products(
                (act, down, hidden, pre), (act_here, down_here, hidden_here, pre_here), in_sem, out_sem, jobs, (1, 2, 4, 5, 7, 8)
            ),
        ]
    )


def reduce_back(size, part, d_out, mid, gain, act, down, hidden, pre):
    rows, width = part.shape
    units = down.shape[0]
    unit = rows // 2 // size
    return pl.pallas_call(
        functools.partial(back_kernel, size, rows, width),
        out_shape=(
            jax.ShapeDtypeStruct((rows, width), jnp.bfloat16),
            jax.ShapeDtypeStruct((2 * unit, width), jnp.float32),
            jax.ShapeDtypeStruct((4, 8, width), jnp.float32),
            jax.ShapeDtypeStruct((rows, width), jnp.bfloat16),
            jax.ShapeDtypeStruct((width, units), jnp.bfloat16),
        ),
        in_specs=[HBM, HBM, VMEM, VMEM, HBM, HBM, HBM, HBM],
        out_specs=(HBM, VMEM, VMEM, HBM, HBM),
        scratch_shapes=stream_scratch(size, rows, width)
        + [pltpu.VMEM((2, unit, width), jnp.bfloat16), pltpu.SemaphoreType.DMA((2,))]
        + [
            pltpu.VMEM((rows, units), jnp.bfloat16),
            pltpu.VMEM((units, width), jnp.bfloat16),
            pltpu.VMEM((rows, width), jnp.bfloat16),
            pltpu.VMEM((rows, units), jnp.bfloat16),
            pltpu.VMEM((rows, width), jnp.bfloat16),
            pltpu.VMEM((width, units), jnp.bfloat16),
            pltpu.VMEM((BLOCK, rows), jnp.bfloat16),
            pltpu.SemaphoreType.DMA((4,)),
            pltpu.SemaphoreType.DMA((2 * (width // BLOCK),)),
        ],
        compiler_params=pltpu.CompilerParams(
            collective_id=2, has_side_effects=True, vmem_limit_bytes=60 * 1024 * 1024
        ),
        name="reduce_back",
    )(part, d_out, mid, gain, act, down, hidden, pre)


def remote_copy(axis, target, src, dst, send_sem, recv_sem):
    return pltpu.make_async_remote_copy(
        src_ref=src,
        dst_ref=dst,
        send_sem=send_sem,
        recv_sem=recv_sem,
        device_id={axis: target},
        device_id_type=pl.DeviceIdType.MESH,
    )


CHUNK = 32
SKEW = 2
CORE_SEND, CORE_RECV, UP_SEND, LEFT_RECV, RIGHT_RECV, BACK_LEFT, BACK_RIGHT, BACK_RECV, TWIN_SEND, TWIN_RECV, KEEP, LOAD = range(12)


def chain_scratch(rows, width):
    half = rows // 2
    return [pltpu.VMEM((half, width), jnp.bfloat16)] * 4 + [pltpu.SemaphoreType.DMA((12, half // CHUNK))]


def chain(devices, sources, out, own, twin, left, right, sems):
    length = devices // 2
    me = lax.axis_index("dp")
    core, place = me % 2, me // 2
    other = me + 1 - 2 * core
    deepest = length // 2

    def at(ref, chunk):
        return ref.at[pl.ds(pl.multiple_of(chunk * CHUNK, CHUNK), CHUNK), :]

    def part(ref, side, chunk):
        return ref.at[pl.ds(pl.multiple_of((2 * chunk + side) * CHUNK, CHUNK), CHUNK), :]

    def core_copy(source, chunk, first):
        return remote_copy("dp", other, part(source, 1 - core, chunk - first), at(twin, chunk), sems.at[CORE_SEND, chunk], sems.at[CORE_RECV, chunk])

    def load(source, chunk, first):
        return pltpu.make_async_copy(part(source, core, chunk - first), at(own, chunk), sems.at[LOAD, chunk])

    def to_right(chunk):
        return remote_copy("dp", me + 2, at(own, chunk), at(left, chunk), sems.at[UP_SEND, chunk], sems.at[LEFT_RECV, chunk])

    def to_left(chunk):
        return remote_copy("dp", me - 2, at(own, chunk), at(right, chunk), sems.at[UP_SEND, chunk], sems.at[RIGHT_RECV, chunk])

    def spread(chunk, src, step, send):
        return remote_copy("dp", me + step, src, part(out, core, chunk), sems.at[send, chunk], sems.at[BACK_RECV, chunk])

    def twin_copy(chunk, src):
        return remote_copy("dp", other, src, part(out, core, chunk), sems.at[TWIN_SEND, chunk], sems.at[TWIN_RECV, chunk])

    def twin_arrival(chunk):
        there = part(out, 1 - core, chunk)
        return remote_copy("dp", other, there, there, sems.at[TWIN_SEND, chunk], sems.at[TWIN_RECV, chunk])

    def keep(chunk):
        return pltpu.make_async_copy(at(own, chunk), part(out, core, chunk), sems.at[KEEP, chunk])

    def add(chunk, terms):
        def strip(step):
            line = pl.ds(pl.multiple_of(chunk * CHUNK + step * STRIP, STRIP), STRIP)
            total = own[line, :].astype(jnp.float32)
            for term in terms:
                total = total + term[line, :].astype(jnp.float32)
            own[line, :] = total.astype(own.dtype)

        pl.loop(0, CHUNK // STRIP)(strip)

    def gather_up(chunk, goal):
        core_copy(out, chunk, 0).wait_recv()
        load(out, chunk, 0).wait()
        has_left = (place > 0) & (place <= goal)
        has_right = (place < length - 1) & (place >= goal)

        @pl.when(~has_right & ~has_left)
        def _():
            add(chunk, [twin])

        @pl.when(has_left & ~has_right)
        def _():
            to_right(chunk).wait_recv()
            add(chunk, [twin, left])

        @pl.when(has_right & ~has_left)
        def _():
            to_left(chunk).wait_recv()
            add(chunk, [twin, right])

        @pl.when(has_left & has_right)
        def _():
            to_right(chunk).wait_recv()
            to_left(chunk).wait_recv()
            add(chunk, [twin, left, right])

        @pl.when(place < goal)
        def _():
            to_right(chunk).start()

        @pl.when(place > goal)
        def _():
            to_left(chunk).start()

        @pl.when(place == goal)
        def _():
            @pl.when(place > 0)
            def _():
                spread(chunk, at(own, chunk), -2, BACK_LEFT).start()

            @pl.when(place < length - 1)
            def _():
                spread(chunk, at(own, chunk), 2, BACK_RIGHT).start()

            twin_copy(chunk, at(own, chunk)).start()
            keep(chunk).start()

    def hand_back(chunk, goal):
        here = part(out, core, chunk)

        @pl.when(place < goal)
        def _():
            spread(chunk, here, 2, BACK_RIGHT).wait_recv()

            @pl.when(place > 0)
            def _():
                spread(chunk, here, -2, BACK_LEFT).start()

            twin_copy(chunk, here).start()

        @pl.when(place > goal)
        def _():
            spread(chunk, here, -2, BACK_LEFT).wait_recv()

            @pl.when(place < length - 1)
            def _():
                spread(chunk, here, 2, BACK_RIGHT).start()

            twin_copy(chunk, here).start()

    def finish(chunk, goal):
        here = part(out, core, chunk)
        core_copy(out, chunk, 0).wait_send()
        twin_arrival(chunk).wait_recv()
        twin_copy(chunk, here).wait_send()

        @pl.when(place < goal)
        def _():
            to_right(chunk).wait_send()

        @pl.when(place > goal)
        def _():
            to_left(chunk).wait_send()

        @pl.when((place <= goal) & (place > 0))
        def _():
            spread(chunk, here, -2, BACK_LEFT).wait_send()

        @pl.when((place >= goal) & (place < length - 1))
        def _():
            spread(chunk, here, 2, BACK_RIGHT).wait_send()

        @pl.when(place == goal)
        def _():
            keep(chunk).wait()

    def open_source(source, first, count):
        @pl.loop(first, first + count)
        def _(chunk):
            core_copy(source, chunk, first).start()
            load(source, chunk, first).start()

    late = []
    first = 0
    for source, rows, before in sources:
        count = rows // 2 // CHUNK
        if before is None:
            open_source(source, first, count)
        else:
            late.append((source, first, count, before))
        first += count
    pairs = first // 2
    yield
    for step in range(pairs + SKEW * 2 * deepest):
        for source, begin, count, before in late:
            if step == max(0, begin // 2 - 2):
                for _ in before:
                    pass
                open_source(source, begin, count)
        for parity in (0, 1):
            goal = deepest - 1 + parity
            below = (place < goal).astype(jnp.int32)
            above = (place > goal).astype(jnp.int32)
            level = below * place + above * (length - 1 - place) + (1 - below - above) * deepest
            pair = step - SKEW * level

            @pl.when((pair >= 0) & (pair < pairs))
            def _(parity=parity, goal=goal, pair=pair):
                gather_up(2 * pair + parity, goal)

            away = below * (goal - place) + above * (place - goal)
            pair_back = step - SKEW * (deepest + away)

            @pl.when((away > 0) & (pair_back >= 0) & (pair_back < pairs))
            def _(parity=parity, goal=goal, pair_back=pair_back):
                hand_back(2 * pair_back + parity, goal)

        yield

    @pl.loop(0, pairs)
    def _(pair):
        finish(2 * pair, deepest - 1)
        finish(2 * pair + 1, deepest)


def small_scratch(size, devices, width):
    return [
        pltpu.VMEM((size, 8, width), jnp.float32),
        pltpu.VMEM((devices, 16, width), jnp.float32),
        pltpu.SemaphoreType.DMA((2, size)),
        pltpu.SemaphoreType.DMA((2, devices)),
    ]


def small_sum(size, devices, turns, given, sums, out, near, far, near_sem, far_sem):
    def send(axis, members, slots, sem):
        me = lax.axis_index(axis)
        copies = []
        for step in range(1, members):
            target = (me + step) % members
            copy = remote_copy(axis, target, slots.at[me], slots.at[me], sem.at[0, target], sem.at[1, me])
            copy.start()
            copies.append(copy)
        return copies

    def receive(axis, members, slots, sem, copies):
        me = lax.axis_index(axis)
        for step in range(1, members):
            source = (me + step) % members
            remote_copy(axis, source, slots.at[source], slots.at[source], sem.at[0, source], sem.at[1, source]).wait_recv()
        for copy in copies:
            copy.wait_send()

    for _ in range(turns):
        yield True
    mine = given[0:8, :]
    row = lax.broadcasted_iota(jnp.int32, mine.shape, 0)
    mine = jnp.where(row == 0, jnp.sum(sums[0], axis=0, keepdims=True), mine)
    mine = jnp.where(row == 1, jnp.sum(sums[1], axis=0, keepdims=True), mine)
    near[lax.axis_index("tensor")] = mine
    copies = send("tensor", size, near, near_sem)
    yield True
    receive("tensor", size, near, near_sem, copies)
    total = near[0]
    for member in range(1, size):
        total = total + near[member]
    me = lax.axis_index("dp")
    far[me, 0:8, :] = total
    far[me, 8:16, :] = given[8:16, :]
    copies = send("dp", devices, far, far_sem)
    yield False
    yield False
    receive("dp", devices, far, far_sem, copies)
    total = far[0]
    for member in range(1, devices):
        total = total + far[member]
    out[...] = total


def in_turns(*parts):
    waiting = list(parts)
    while waiting:
        left = []
        for one, quiet in waiting:
            ended = False
            try:
                while not ended:
                    ended = next(one)
                    if not quiet:
                        yield
                left.append((one, quiet))
            except StopIteration:
                pass
        waiting = left


def greet_all(sizes):
    barrier = pltpu.get_barrier_semaphore()
    total = 0
    for axis, size in sizes:
        me = lax.axis_index(axis)
        for step in range(1, size):
            pl.semaphore_signal(
                barrier, inc=1, device_id={axis: (me + step) % size}, device_id_type=pl.DeviceIdType.MESH
            )
        total += size - 1
    pl.semaphore_wait(barrier, total)


def last_kernel(size, devices, shapes, mlp, part, kv, tokens, mid, dmid, dbias, gain, small, *rest):
    wide, kv_shape, summed = shapes[0], shapes[1], shapes[2:]
    arrays, rest = rest[: len(summed)], rest[len(summed) :]
    result, grad, total, small_out, kv_out, rest = *rest[:5], rest[5:]
    first, second, third, rest = rest[:6], rest[6:12], rest[12:18], rest[18:]
    tok, load_sem, sums, rest = *rest[:3], rest[3:]
    greet_all((("tensor", size), ("dp", devices)))
    loads = load_rows("tensor", size, wide[0], tokens, tok, load_sem)
    sums[...] = jnp.zeros_like(sums)

    def finish_result(total, number, here, line):
        return (mid[line, :] + total + dbias[...]).astype(jnp.bfloat16)

    def finish_grad(total, number, here, line):
        scaled, scale = moments(tok[number, here, :].astype(jnp.float32))
        sums[0] += fold(total * scaled)
        sums[1] += fold(total)
        return (dmid[line, :] + norm_back(total, gain[...], scaled, scale)).astype(jnp.bfloat16)

    def finish_kv(total, number, here, line):
        return total.astype(jnp.bfloat16)

    kv_stream = stream("tensor", size, kv_shape, kv, kv_out, *third, finish_kv)
    sources = [(array, shape[0], None) for array, shape in zip(arrays, summed)]
    sources.append((kv_out, kv_shape[0], kv_stream))
    run_together(
        [
            in_turns(
                (kv_stream, True),
                (stream("tensor", size, wide, part, grad, *second, finish_grad, loads), False),
                (stream("tensor", size, wide, mlp, result, *first, finish_result), False),
                (small_sum(size, devices, size.bit_length() - 1, small, sums, small_out, *rest[:4]), False),
            ),
            chain(devices, sources, total, *rest[4:]),
        ]
    )


def reduce_last(size, devices, mlp, part, kv, tokens, mid, dmid, dbias, gain, small, arrays):
    rows, width = part.shape
    unit = rows // 2 // size
    shapes = (part.shape, kv.shape) + tuple(array.shape for array in arrays)
    lines = sum(shape[0] for shape in shapes[1:])
    low = jnp.bfloat16
    return pl.pallas_call(
        functools.partial(last_kernel, size, devices, shapes),
        out_shape=(
            jax.ShapeDtypeStruct((rows, width), low),
            jax.ShapeDtypeStruct((rows, width), low),
            jax.ShapeDtypeStruct((lines, width), low),
            jax.ShapeDtypeStruct(small.shape, jnp.float32),
            jax.ShapeDtypeStruct(kv.shape, low),
        ),
        in_specs=[HBM] * 4 + [VMEM] * 5 + [HBM] * len(arrays),
        out_specs=(HBM, HBM, HBM, VMEM, HBM),
        scratch_shapes=stream_scratch(size, rows, width) * 2
        + stream_scratch(size, kv.shape[0], width)
        + [
            pltpu.VMEM((2, unit, width), low),
            pltpu.SemaphoreType.DMA((2,)),
            pltpu.VMEM((2, 8, width), jnp.float32),
        ]
        + small_scratch(size, devices, width)
        + chain_scratch(lines, width),
        compiler_params=pltpu.CompilerParams(
            collective_id=3, has_side_effects=True, vmem_limit_bytes=60 * 1024 * 1024
        ),
        name="reduce_last",
    )(mlp, part, kv, tokens, mid, dmid, dbias, gain, small, *arrays)[:4]


def layer_norm(values, gain, shift):
    center = values - jnp.mean(values, axis=-1, keepdims=True)
    scaled = center * lax.rsqrt(jnp.mean(center * center, axis=-1, keepdims=True) + 1e-05)
    return scaled * gain + shift


def gelu_tanh(values):
    return (
        0.5
        * values
        * (1.0 + jnp.tanh(0.7978845608028654 * (values + 0.044715 * values * values * values)))
    )


def contract_rows(left, right):
    return lax.dot_general(
        left, right, (((0,), (0,)), ((), ())), preferred_element_type=jnp.float32
    )


def contract_cols(left, right):
    return lax.dot_general(
        left, right, (((1,), (1,)), ((), ())), preferred_element_type=jnp.float32
    )


def block_scores(query_block, key_rows, offset, length):
    scale = query_block.shape[2] ** (-0.5)
    scores = (
        jnp.einsum("qhd,kd->hqk", query_block, key_rows, preferred_element_type=jnp.float32) * scale
    )
    rows_pos = offset + jnp.arange(query_block.shape[0], dtype=jnp.int32)
    keys_pos = jnp.arange(key_rows.shape[0], dtype=jnp.int32)
    allowed = (keys_pos[None, :] <= rows_pos[:, None]) & (keys_pos[None, :] < length)
    return jnp.where(allowed[None], scores, -1e30)


def attend_forward(queries, key_rows, value_rows, length, block_rows):
    pieces = []
    log_totals = []
    for offset in range(0, queries.shape[0], block_rows):
        query_block = queries[offset : offset + block_rows]
        scores = block_scores(query_block, key_rows, offset, length)
        highest = jnp.max(scores, axis=-1, keepdims=True)
        exponent = jnp.exp(scores - highest)
        normaliser = jnp.sum(exponent, axis=-1, keepdims=True)
        probability = (exponent / normaliser).astype(jnp.bfloat16)
        log_totals.append(highest + jnp.log(normaliser))
        pieces.append(
            jnp.einsum("hqk,kd->qhd", probability, value_rows, preferred_element_type=jnp.float32)
        )
    return (jnp.concatenate(pieces, axis=0), log_totals)


def attend_backward(queries, key_rows, value_rows, length, block_rows, log_totals, grad_heads):
    scale = queries.shape[2] ** (-0.5)
    query_grads = []
    key_grads = jnp.zeros(key_rows.shape, jnp.float32)
    value_grads = jnp.zeros(value_rows.shape, jnp.float32)
    for counter, offset in enumerate(range(0, queries.shape[0], block_rows)):
        query_block = queries[offset : offset + block_rows]
        grad_block = grad_heads[offset : offset + block_rows]
        scores = block_scores(query_block, key_rows, offset, length)
        probability = jnp.exp(scores - log_totals[counter])
        grad_probs = jnp.einsum(
            "qhd,kd->hqk", grad_block, value_rows, preferred_element_type=jnp.float32
        )
        inner = jnp.sum(probability * grad_probs, axis=-1, keepdims=True)
        grad_scores = (probability * (grad_probs - inner)).astype(jnp.bfloat16)
        query_grads.append(
            (
                jnp.einsum("hqk,kd->qhd", grad_scores, key_rows, preferred_element_type=jnp.float32)
                * scale
            ).astype(jnp.bfloat16)
        )
        key_grads = (
            key_grads
            + jnp.einsum(
                "hqk,qhd->kd", grad_scores, query_block, preferred_element_type=jnp.float32
            )
            * scale
        )
        value_grads = value_grads + jnp.einsum(
            "hqk,qhd->kd",
            probability.astype(jnp.bfloat16),
            grad_block,
            preferred_element_type=jnp.float32,
        )
    return (jnp.concatenate(query_grads, axis=0), key_grads, value_grads)


def local(
    size,
    devices,
    tokens,
    lengths,
    norm1_gain,
    norm1_shift,
    query_weight,
    query_bias,
    keyval_weight,
    value_bias,
    proj_weight,
    proj_bias,
    norm2_gain,
    norm2_shift,
    up_weight,
    up_bias,
    down_weight,
    down_bias,
    cotangent,
):
    wide = jnp.float32
    slot_len, width = tokens.shape
    head_dim = keyval_weight.shape[1] // 2
    heads_here = query_weight.shape[1] // head_dim
    block_rows = min(512, slot_len)
    length = lengths[0]

    def row(vector):
        return vector.astype(wide).reshape(1, -1)

    hidden1 = layer_norm(tokens.astype(wide), norm1_gain.astype(wide), norm1_shift.astype(wide)).astype(jnp.bfloat16)
    queries = (
        jnp.dot(hidden1, query_weight, preferred_element_type=wide) + query_bias.astype(wide)
    ).astype(jnp.bfloat16)
    keyval = jnp.dot(hidden1, keyval_weight, preferred_element_type=wide)
    key_rows = keyval[:, :head_dim].astype(jnp.bfloat16)
    value_rows = (keyval[:, head_dim:] + value_bias.astype(wide)).astype(jnp.bfloat16)
    slot_queries = queries.reshape(slot_len, heads_here, head_dim)
    attended, log_totals = attend_forward(slot_queries, key_rows, value_rows, length, block_rows)
    heads_out = attended.reshape(slot_len, heads_here * head_dim).astype(jnp.bfloat16)
    attn_terms = jnp.dot(heads_out, proj_weight, preferred_element_type=wide).astype(jnp.bfloat16)
    valid = (jnp.arange(slot_len, dtype=jnp.int32) < length)[:, None]
    d_out = jnp.where(valid, cotangent, jnp.zeros_like(cotangent))
    hidden2, mid, grad_act = reduce_middle(
        size, attn_terms, tokens, row(proj_bias), row(norm2_gain), row(norm2_shift), d_out, down_weight
    )

    pre_act = jnp.dot(hidden2, up_weight, preferred_element_type=wide) + up_bias.astype(wide)
    activated = gelu_tanh(pre_act).astype(jnp.bfloat16)
    grad_down = contract_rows(activated, d_out).astype(jnp.bfloat16)
    grad_down = lax.psum(grad_down, "dp")
    gelu_pull = jax.vjp(gelu_tanh, pre_act)[1]
    grad_pre = gelu_pull(grad_act.astype(wide))[0].astype(jnp.bfloat16)
    back2 = contract_cols(grad_pre, up_weight).astype(jnp.bfloat16)
    middle_low, dmid, sums2, mlp_terms, grad_up = reduce_back(
        size, back2, d_out, mid, row(norm2_gain), activated, down_weight, hidden2, grad_pre
    )
    if up_weight.shape[1] != width:
        grad_up = grad_up.T
    grad_upbias = jnp.sum(grad_pre.astype(wide), axis=0)

    grad_proj = contract_rows(heads_out, middle_low).astype(jnp.bfloat16)
    grad_heads = contract_cols(middle_low, proj_weight).astype(jnp.bfloat16)
    slot_grads = grad_heads.reshape(slot_len, heads_here, head_dim)
    query_part, key_part, value_part = attend_backward(
        slot_queries, key_rows, value_rows, length, block_rows, log_totals, slot_grads
    )
    grad_queries = query_part.reshape(slot_len, heads_here * head_dim)
    grad_kv_rows = jnp.concatenate([key_part, value_part], axis=1).astype(jnp.bfloat16)
    grad_qbias = jnp.sum(grad_queries.astype(wide), axis=0)
    grad_query = contract_rows(grad_queries, hidden1).astype(jnp.bfloat16)
    grad_keyval = contract_rows(grad_kv_rows, hidden1).astype(jnp.bfloat16)
    grad_vbias = jnp.sum(grad_kv_rows[:, head_dim:].astype(wide), axis=0)
    back1 = (
        contract_cols(grad_queries, query_weight) + contract_cols(grad_kv_rows, keyval_weight)
    ).astype(jnp.bfloat16)

    def padded(vector):
        return jnp.pad(vector, (0, width - vector.shape[0])).reshape(1, width)

    small = jnp.concatenate(
        [
            jnp.zeros((2, width), wide),
            jnp.sum(sums2, axis=1),
            padded(grad_vbias),
            jnp.zeros((1, width), wide),
            padded(grad_qbias),
            padded(grad_upbias),
            jnp.zeros((6, width), wide),
        ]
    )
    arrays = (grad_up, grad_proj, grad_query, grad_keyval)
    result, grad_tokens, total, small = reduce_last(
        size,
        devices,
        mlp_terms,
        back1,
        grad_keyval,
        tokens,
        mid,
        dmid,
        row(down_bias),
        row(norm1_gain),
        small,
        arrays[:3],
    )
    ends = [0]
    for array in arrays:
        ends.append(ends[-1] + array.shape[0])
    grad_up, grad_proj, grad_query, kv_sum = (total[low:high] for low, high in zip(ends, ends[1:]))
    grad_up = widen(total, 0, ends[1])
    if up_weight.shape[1] != width:
        grad_up = grad_up.T
    grad_gain1, grad_shift1, grad_gain2, grad_shift2, grad_pbias, grad_dnbias = (
        small[place] for place in range(6)
    )
    grad_vbias = small[6, :head_dim]
    grad_qbias = small[8, : query_bias.shape[0]]
    grad_upbias = small[9, : up_bias.shape[0]]
    return (
        result,
        grad_tokens,
        grad_gain1,
        grad_shift1,
        grad_query.T.astype(wide),
        grad_qbias,
        kv_sum.T.astype(wide),
        grad_vbias,
        grad_proj.astype(wide),
        grad_pbias,
        grad_gain2,
        grad_shift2,
        grad_up,
        grad_upbias,
        widen(grad_down, 0, grad_down.shape[0]),
        grad_dnbias,
    )


def solution(mesh):
    in_specs = (
        P("dp", None),
        P("dp"),
        P(),
        P(),
        P(None, "tensor"),
        P("tensor"),
        P(),
        P(),
        P("tensor", None),
        P(),
        P(),
        P(),
        P(None, "tensor"),
        P("tensor"),
        P("tensor", None),
        P(),
        P("dp", None),
    )
    out_specs = (
        P("dp", None),
        P("dp", None),
        P(),
        P(),
        P(None, "tensor"),
        P("tensor"),
        P(),
        P(),
        P("tensor", None),
        P(),
        P(),
        P(),
        P(None, "tensor"),
        P("tensor"),
        P("tensor", None),
        P(),
    )
    return jax.shard_map(functools.partial(local, mesh.shape["tensor"], mesh.shape["dp"]), mesh=mesh, in_specs=in_specs, out_specs=out_specs, check_vma=False)
```
